256 devices in a mesh: gx: 4 (over z_hi), gy: 4 (over y), gz: 16 (over x, z_lo, core).
Axes of the slice: x: 4, y: 4, z: 8 (z_hi: 4, z_lo: 2; z = z_hi * 2 + z_lo), core: 2. Of those that a mesh axis runs over, the one named last changes fastest.
Arguments:
- volume: float32 [256, 256, 4096], P('gz', 'gy', 'gx'), may hold values from -24 to 24
Outputs:
- level_one: float32 [128, 128, 2048], P('gz', 'gy', 'gx')
- level_two: float32 [64, 64, 1024], P('gz', 'gy', 'gx')
- level_three: float32 [32, 32, 512], P('gz', 'gy', 'gx')
The draws below stay inside these ranges and needn't reach their ends.
All inputs are finite; a program needn't handle non-finite values.
Results may differ from the reference program's by a relative error of at most 0.00002.
Values sent between devices are 32-bit elements; how exact they have to be, the bound alone decides.
No kernel may reach another device: no remote copies, remote signals or barrier semaphores. Data moves between devices by JAX's collectives and lax.ppermute only.
A program may use at most 64 MiB of HBM per device.

```python
import jax
import jax.numpy as jnp
from jax import lax

NX = 4096
NY = 256
NZ = 256


def shard_levels(stream_key, shape, split, smallest, largest):
    level = 1.0
    for dim, shards_of in split:
        draws = jax.random.uniform(jax.random.fold_in(jax.random.fold_in(stream_key, 6), dim), (shards_of,), jnp.float32, smallest / len(split), largest / len(split))
        level = level * jnp.repeat(jnp.exp(draws), shape[dim] // shards_of).reshape((-1,) + (1,) * (len(shape) - 1 - dim))
    return level


def gaussian(rng, dims, deviation, most, cuts=(), kind=jnp.bfloat16):
    result = deviation * jax.random.normal(rng, dims, jnp.float32)
    if cuts:
        result = result * shard_levels(rng, dims, cuts, -0.22, 0.18)
    return jnp.clip(result, -most, most).astype(kind)


def setup_inputs(seed: int = 0) -> dict:
    streams_of = jax.random.split(jax.random.key(seed), 2)
    return {
        "volume": gaussian(streams_of[0], (NZ, NY, NX), 4.0, 24.0, ((0, 16), (1, 4), (2, 4)), jnp.float32),
    }


taps = (0.0625, 0.25, 0.375, 0.25, 0.0625)


def reduce_padded(padded, dim, count):
    total = None
    for k in range(5):
        piece = lax.slice_in_dim(padded, k, k + 2 * count - 1, 2, dim)
        term = taps[k] * piece
        total = term if total is None else total + term
    return total


def reduce_axis(field, dim):
    widths = [(0, 0), (0, 0), (0, 0)]
    widths[dim] = (2, 2)
    padded = jnp.pad(field, widths)
    return reduce_padded(padded, dim, field.shape[dim] // 2)


def level_down(field):
    return reduce_axis(reduce_axis(reduce_axis(field, 0), 1), 2)


def reference(volume):
    level_one = level_down(volume)
    level_two = level_down(level_one)
    level_three = level_down(level_two)
    return level_one, level_two, level_three
```

```python
import numpy as np
import jax
import jax.numpy as jnp
from jax import lax
from jax.experimental import pallas as pl
from jax.experimental.pallas import tpu as pltpu
from jax.sharding import PartitionSpec as P

taps = (0.0625, 0.25, 0.375, 0.25, 0.0625)
f32, bf16 = jnp.float32, jnp.bfloat16
VMEM = pl.BlockSpec(memory_space=pltpu.VMEM)


def column_weights():
    w = np.zeros((256, 256), np.float32)
    for i in range(-1, 129):
        for k in range(5):
            c = 2 * i - 2 + k
            if 0 <= c < 256:
                lane = i if 0 <= i < 128 else (128 if i == 128 else 255)
                w[c, lane] += taps[k]
    return np.concatenate([w] * 3, axis=0)


def edge_weights():
    w = np.zeros((128, 256), np.float32)
    for c in range(128):
        for k in range(5):
            place = c - 128 if c >= 64 else c
            if (place + 2 - k) % 2:
                continue
            i = (place + 2 - k) // 2
            if c >= 64:
                lane = 128 + i if i < 0 else 128 + i
                w[c, lane] += taps[k]
            else:
                lane = i if i >= 0 else 256 + i
                w[c, lane] += taps[k]
    return np.concatenate([w] * 3, axis=0)


def composite(levels):
    h = np.ones(1)
    for level in range(levels):
        up = np.zeros(4 * 2**level + 1)
        up[:: 2**level] = taps
        h = np.convolve(h, up)
    return h


def shell_weights():
    rows = [(1, 0), (2, 0), (2, 1), (3, 0), (3, 1), (1, -1), (2, -1), (3, -1)]
    w = np.zeros((8, 256), np.float64)
    for r, (level, place) in enumerate(rows):
        h = composite(level)
        reach = len(h) // 2
        for t in range(len(h)):
            c = place * 2**level + t - reach
            if r < 5 and -128 <= c < 0:
                w[r, 256 + c] = h[t]
            if r >= 5 and 0 <= c < 128:
                w[r, c] = h[t]
    high = w.astype(jnp.bfloat16).astype(np.float64)
    return np.concatenate([high, w - high], axis=0).astype(np.float32)


def split(x):
    a = x.astype(bf16)
    r = x - a.astype(f32)
    b = r.astype(bf16)
    return a, b, (r - b.astype(f32)).astype(bf16)


def weigh(p):
    total = None
    for a, b, t in ((p[0], p[4], taps[0]), (p[1], p[3], taps[1]), (p[2], None, taps[2])):
        if a is None and b is None:
            continue
        s = a if b is None else b if a is None else a + b
        total = t * s if total is None else total + t * s
    return total


def keep(axis, count):
    at = lax.axis_index(axis)
    return (
        jnp.where(at > 0, 1.0, 0.0).astype(f32),
        jnp.where(at < count - 1, 1.0, 0.0).astype(f32),
    )


def sections(load, store, first, last, half, above, ends):
    got = {i: load(i) for i in range(first, last + 1)}
    for i in range(-1, half + above):
        v = weigh([got.get(2 * i - 2 + k) for k in range(5)])
        if i < 0:
            v = v * ends[0]
        if i >= half:
            v = v * ends[1]
        store(i, v)


def rows(src, dst, at, half, above, ends):
    n = 2 * half
    dst[at, 8 : 8 + half, :] = weigh(
        [src[at, pl.ds(6 + k, half, stride=2), :] for k in range(5)]
    )
    low = taps[3] * src[at, 7:8, :] + taps[4] * src[at, 8:9, :]
    dst[at, 0:8, :] = jnp.where(
        lax.broadcasted_iota(jnp.int32, (8, 128), 0) == 7, low * ends[0], 0.0
    )
    up = [src[at, 6 + n + k : 7 + n + k, :] for k in range(4)]
    high = weigh(up + [None]) * ends[1]
    higher = (taps[0] * up[2] + taps[1] * up[3]) * ends[1]
    row = lax.broadcasted_iota(jnp.int32, (8, 128), 0)
    dst[at, 8 + half : 16 + half, :] = jnp.where(row == 0, high, jnp.where(row == 1, higher, 0.0))


def pack(parts, dst, at):
    wide = len(parts) * 128
    tall = parts[0].shape[0]
    for j, x in enumerate(parts):
        for q, piece in enumerate(split(x)):
            dst[at : at + tall, q * wide + j * 128 : q * wide + (j + 1) * 128] = piece


def lane():
    return lax.broadcasted_iota(jnp.int32, (8, 128), 1)


def low_lanes(tall):
    return lax.broadcasted_iota(jnp.int32, (tall, 128), 1) < 64


def matmul(x, w):
    return jnp.dot(x, w, preferred_element_type=f32)


def shell_kernel(left, right, w, out):
    x = jnp.concatenate([left[...].reshape(1024, 128), right[...].reshape(1024, 128)], axis=1)
    total = None
    for piece in split(x):
        t = lax.dot_general(w[...], piece, (((1,), (1,)), ((), ())), preferred_element_type=f32)
        total = t if total is None else total + t
    out[...] = total[:8] + total[8:]


def level_one_block(volume, at, zs, ys, ops, res, w, zend, yend):
    for h in range(2):
        cols = pl.ds(at * 256 + h * 128, 128)
        for s in range(10):
            zs[h, s, 0:8, :] = jnp.zeros((8, 128), f32)
            zs[h, s, 72:80, :] = jnp.zeros((8, 128), f32)
        for r in range(0, 64, 8):

            def store(i, v, r=r, h=h):
                zs[h, i + 1, 8 + r : 16 + r, :] = v

            sections(lambda i, r=r, cols=cols: volume[i, r : r + 8, cols], store, 0, 15, 8, 1, zend)
    for s in range(10):
        for h in range(2):
            rows(zs.at[h], ys.at[h], s, 32, 1, yend)
        pack([ys[0, s], ys[1, s]], ops, s * 48)
    res[...] = matmul(ops[...], w[...])


def first_kernel(volume, w, ea, side, zs, ys, ops, res):
    zend, yend = keep("gz", lax.axis_size("gz")), keep("gy", lax.axis_size("gy"))
    low = low_lanes(48)
    for b in range(2):
        level_one_block(volume, b, zs, ys, ops, res, w, zend, yend)
        for s in range(10):
            main = res[s * 48 : s * 48 + 48, :128]
            beside = res[s * 48 : s * 48 + 48, 128:]
            if b == 0:
                ea[0, s] = main
                side[s] = beside
            else:
                first = side[s]
                ea[1, s] = main + jnp.where(low, first, 0.0)
                ea[0, s] = ea[0, s] + jnp.where(low, 0.0, beside)
                side[s] = jnp.where(low, beside, first)


def next_level(blocks, edge, zs, ys, ops, edge_ops, res, edge_res, w, we, dst, edge_dst,
               sections_in, half_z, half_y, tall_in, used_in, tall, zend, yend, xend):
    count = len(blocks)
    many = half_z + 3
    for j, src in enumerate(blocks + [edge]):
        for r in range(0, used_in, 8):

            def store(i, v, r=r, j=j):
                zs[j, i + 1, r : r + 8, :] = v

            sections(lambda i, r=r, src=src: src[i + 1, r : r + 8, :], store, -1,
                     sections_in - 2, half_z, 2, zend)
        for s in range(many):
            rows(zs.at[j], ys.at[j], s, half_y, 2, yend)
    size = many * tall
    for p in range(count // 2):
        for s in range(many):
            pack([ys[2 * p, s], ys[2 * p + 1, s]], ops, p * size + s * tall)
    for s in range(many):
        pack([ys[count, s]], edge_ops, s * tall)
    res[...] = matmul(ops[...], w[...])
    edge_res[...] = matmul(edge_ops[...], we[...])
    low = low_lanes(tall)
    last = count // 2 - 1
    for s in range(many):
        mains, besides = [], []
        for p in range(last + 1):
            at = p * size + s * tall
            mains.append(res[at : at + tall, :128])
            besides.append(res[at : at + tall, 128:])
        at = s * tall
        edge_beside = edge_res[at : at + tall, 128:]
        for p in range(last + 1):
            under = besides[p - 1] if p else edge_beside
            over = besides[p + 1] if p < last else edge_beside
            dst[p, s] = mains[p] + jnp.where(low, under, over)
        if edge_dst is not None:
            wrapped = edge_res[at : at + tall, :128] + jnp.where(low, besides[last], besides[0])
            edge_dst[s] = wrapped * jnp.where(low, xend[1], xend[0])


def second_kernel(volume, w, we, ea_in, side, ea, eb, f2, f3,
                  zs, ys, ops, res, h1, z2, y2, ops2, opse2, res2, rese2, h2,
                  z3, y3, ops3, opse3, res3, rese3):
    zend, yend, xend = (keep(a, lax.axis_size(a)) for a in ("gz", "gy", "gx"))
    low = low_lanes(48)
    ea[0] = ea_in[0]
    for b in range(2):
        level_one_block(volume, 2 + b, zs, ys, ops, res, w, zend, yend)
        for s in range(10):
            main = res[s * 48 : s * 48 + 48, :128]
            beside = res[s * 48 : s * 48 + 48, 128:]
            if b == 0:
                eb[0, s] = main + jnp.where(low, side[s], 0.0)
                ea[1, s] = ea_in[1, s] + jnp.where(low, 0.0, beside)
                h1[s] = beside
            else:
                eb[1, s] = main + jnp.where(low, h1[s], 0.0)
                eb[0, s] = eb[0, s] + jnp.where(low, 0.0, beside)
                h1[s] = jnp.where(low, beside * xend[1], side[s] * xend[0])
    next_level([ea.at[0], ea.at[1], eb.at[0], eb.at[1]], h1, z2, y2, ops2, opse2, res2, rese2,
               w, we, f2, h2, 10, 4, 16, 48, 48, 32, zend, yend, xend)
    next_level([f2.at[0], f2.at[1]], h2, z3, y3, ops3, opse3, res3, rese3,
               w, we, f3, None, 7, 2, 8, 32, 32, 32, zend, yend, xend)


def route(x, base, tall):
    at = lax.broadcasted_iota(jnp.int32, (tall, 128), 1)
    first, count, last = base
    head = x if first == 0 else pltpu.roll(x, 128 - first, axis=1)
    tail = pltpu.roll(x, 127 - last, axis=1)
    return jnp.where(at < count, head, 0.0), jnp.where(at == 127, tail, 0.0)


def columns_kernel(pa, pb, ea_in, eb_in, f2_in, f3_in, ea, eb, f2, f3, ya, yb,
                   flat, zs, y1, z2, y2, z3, y3):
    zend, yend = keep("gz", lax.axis_size("gz")), keep("gy", lax.axis_size("gy"))
    odd = lax.rem(lax.axis_index("gx"), 2) == 1
    row = lax.broadcasted_iota(jnp.int32, (8, 128), 0)
    for j in range(8):
        a, b = pa[:, j * 128 : j * 128 + 128], pb[:, j * 128 : j * 128 + 128]
        under, over = jnp.where(odd, a, b), jnp.where(odd, b, a)
        mine = jnp.where(row < 5, under, over)
        full = jnp.concatenate([mine, jnp.zeros((120, 128), f32)], axis=0)
        flat[2 * j : 2 * j + 2] = full.T.reshape(2, 64, 128)
    for s in range(10):
        zs[s, 0:8, :] = jnp.zeros((8, 128), f32)
        zs[s, 72:80, :] = jnp.zeros((8, 128), f32)
    for r in range(0, 64, 8):

        def store(i, v, r=r):
            zs[i + 1, 8 + r : 16 + r, :] = v

        sections(lambda i, r=r: flat[i, r : r + 8, :], store, 0, 15, 8, 1, zend)
    for s in range(10):
        rows(zs, y1, s, 32, 1, yend)
        head, tail = route(y1[s], (0, 1, 5), 48)
        ea[0, s] = ea_in[0, s] + head
        eb[1, s] = eb_in[1, s] + tail
        ea[1, s] = ea_in[1, s]
        eb[0, s] = eb_in[0, s]
    for r in range(0, 48, 8):

        def store(i, v, r=r):
            z2[i + 1, r : r + 8, :] = v

        sections(lambda i, r=r: y1[i + 1, r : r + 8, :], store, -1, 8, 4, 2, zend)
    for s in range(7):
        rows(z2, y2, s, 16, 2, yend)
        head, tail = route(y2[s], (1, 2, 6), 32)
        f2[0, s] = f2_in[0, s] + head
        f2[1, s] = f2_in[1, s] + tail
    for r in range(0, 32, 8):

        def store(i, v, r=r):
            z3[i + 1, r : r + 8, :] = v

        sections(lambda i, r=r: y2[i + 1, r : r + 8, :], store, -1, 5, 2, 2, zend)
    for s in range(5):
        rows(z3, y3, s, 8, 2, yend)
        head, tail = route(y3[s], (3, 2, 7), 32)
        f3[0, s] = f3_in[0, s] + head + tail

    def emit(dst, high):
        for blk in range(4):
            e = ea if blk < 2 else eb
            for s in range(10):
                at = 40 if high else 7
                dst[blk * 10 + s : blk * 10 + s + 1, :] = e[blk % 2, s, at : at + 1, :]
        for j in range(2 if high else 1):
            for blk in range(2):
                for s in range(7):
                    at, to = 24 + j if high else 7, 40 + j * 14 + blk * 7 + s
                    dst[to : to + 1, :] = f2[blk, s, at : at + 1, :]
            for s in range(5):
                at, to = 16 + j if high else 7, 68 + j * 5 + s
                dst[to : to + 1, :] = f3[0, s, at : at + 1, :]

    odd_row = lax.rem(lax.axis_index("gy"), 2) == 1
    for dst, when in ((ya, odd_row), (yb, jnp.logical_not(odd_row))):
        pl.when(when)(lambda dst=dst: emit(dst, False))
        pl.when(jnp.logical_not(when))(lambda dst=dst: emit(dst, True))


def rows_kernel(pa, pb, ea_in, eb_in, f2_in, f3_in, ea, eb, f2, f3, za, zb):
    odd = lax.rem(lax.axis_index("gy"), 2) == 1
    ea[...], eb[...], f2[...], f3[...] = ea_in[...], eb_in[...], f2_in[...], f3_in[...]

    def got(at):
        a, b = pa[at : at + 1, :], pb[at : at + 1, :]
        return jnp.where(odd, a, b), jnp.where(odd, b, a)

    def add(ref, blk, s, at, v):
        ref[blk, s, at : at + 1, :] = ref[blk, s, at : at + 1, :] + v

    for blk in range(4):
        e = ea if blk < 2 else eb
        for s in range(10):
            under, over = got(blk * 10 + s)
            add(e, blk % 2, s, 8, under)
            add(e, blk % 2, s, 39, over)
    for j in range(2):
        for blk in range(2):
            for s in range(7):
                under, over = got(40 + j * 14 + blk * 7 + s)
                add(f2, blk, s, 8 + j, under)
                if j == 0:
                    add(f2, blk, s, 23, over)
        for s in range(5):
            under, over = got(68 + j * 5 + s)
            add(f3, 0, s, 8 + j, under)
            if j == 0:
                add(f3, 0, s, 15, over)

    def emit(dst, high):
        for blk in range(4):
            e = ea if blk < 2 else eb
            dst[blk * 32 : blk * 32 + 32, :] = e[blk % 2, 9 if high else 0, 8:40, :]
        for j in range(2 if high else 1):
            for blk in range(2):
                to = 128 + j * 32 + blk * 16
                dst[to : to + 16, :] = f2[blk, 5 + j if high else 0, 8:24, :]
            to = 192 + j * 8
            dst[to : to + 8, :] = f3[0, 3 + j if high else 0, 8:16, :]

    odd_slab = lax.rem(lax.axis_index("gz"), 2) == 1
    for dst, when in ((za, odd_slab), (zb, jnp.logical_not(odd_slab))):
        pl.when(when)(lambda dst=dst: emit(dst, False))
        pl.when(jnp.logical_not(when))(lambda dst=dst: emit(dst, True))


def sections_kernel(pa, pb, ea, eb, f2, f3, one, two, three):
    odd = lax.rem(lax.axis_index("gz"), 2) == 1

    def got(at, tall):
        a, b = pa[at : at + tall, :], pb[at : at + tall, :]
        return jnp.where(odd, a, b), jnp.where(odd, b, a)

    for blk in range(4):
        e = ea if blk < 2 else eb
        under, over = got(blk * 32, 32)
        for z in range(8):
            v = e[blk % 2, z + 1, 8:40, :]
            v = v + under if z == 0 else v + over if z == 7 else v
            one[z, :, blk * 128 : blk * 128 + 128] = v
    for blk in range(2):
        under, over = got(128 + blk * 16, 16)
        further, _ = got(160 + blk * 16, 16)
        for z in range(4):
            v = f2[blk, z + 1, 8:24, :]
            v = v + under if z == 0 else v + further if z == 1 else v + over if z == 3 else v
            two[z, :, blk * 128 : blk * 128 + 128] = v
    under, over = got(192, 8)
    further, _ = got(200, 8)
    three[0] = f3[0, 1, 8:16, :] + under
    three[1] = f3[0, 2, 8:16, :] + further + over


def shape(*dims):
    return jax.ShapeDtypeStruct(dims, f32)


def swap(x, axis, first):
    count = lax.axis_size(axis)
    pairs = []
    for i in range(first, count - 1, 2):
        pairs += [(i, i + 1), (i + 1, i)]
    return lax.ppermute(x, axis, pairs)


def call(kernel, outs, scratch, args, name, flops, moved, specs=None, aliases=None):
    return pl.pallas_call(
        kernel,
        out_shape=outs,
        in_specs=specs or [VMEM] * len(args),
        out_specs=[VMEM] * len(outs),
        scratch_shapes=scratch,
        input_output_aliases=aliases or {},
        cost_estimate=pl.CostEstimate(flops=flops, bytes_accessed=moved, transcendentals=0),
        name=name,
    )(*args)


def on_device(volume):
    w = jnp.asarray(column_weights(), bf16)
    we = jnp.asarray(edge_weights(), bf16)
    ws = jnp.asarray(shell_weights(), bf16)
    buf = pltpu.VMEM
    shells = pl.pallas_call(
        shell_kernel,
        grid=(1,),
        out_shape=shape(8, 1024),
        in_specs=[
            pl.BlockSpec((16, 64, 128), lambda i: (0, 0, 0)),
            pl.BlockSpec((16, 64, 128), lambda i: (0, 0, 7)),
            pl.BlockSpec((16, 256), lambda i: (0, 0)),
        ],
        out_specs=pl.BlockSpec((8, 1024), lambda i: (0, 0)),
        cost_estimate=pl.CostEstimate(flops=10**8, bytes_accessed=1 << 20, transcendentals=0),
        name="shells",
    )(volume, volume, ws)
    xa = swap(shells, "gx", 0)
    xb = swap(shells, "gx", 1)
    block = [buf((2, 10, 80, 128), f32), buf((2, 10, 48, 128), f32), buf((480, 768), bf16), buf((480, 256), f32)]
    e, f2s, f3s = shape(2, 10, 48, 128), shape(2, 7, 32, 128), shape(1, 5, 32, 128)
    ea, side = call(first_kernel, [e, shape(10, 48, 128)], block, (volume, w), "first", 4 * 10**9, 1 << 21)
    ea, eb, f2, f3 = call(
        second_kernel,
        [e, e, f2s, f3s],
        block
        + [buf((10, 48, 128), f32)]
        + [buf((5, 7, 48, 128), f32), buf((5, 7, 32, 128), f32), buf((448, 768), bf16), buf((224, 384), bf16)]
        + [buf((448, 256), f32), buf((224, 256), f32), buf((7, 32, 128), f32)]
        + [buf((3, 5, 32, 128), f32), buf((3, 5, 32, 128), f32), buf((160, 768), bf16), buf((160, 384), bf16)]
        + [buf((160, 256), f32), buf((160, 256), f32)],
        (volume, w, we, ea, side),
        "second",
        5 * 10**9,
        1 << 21,
    )
    keepers = {2: 0, 3: 1, 4: 2, 5: 3}
    ea, eb, f2, f3, ya, yb = call(
        columns_kernel,
        [e, e, f2s, f3s, shape(80, 128), shape(80, 128)],
        [buf((16, 64, 128), f32), buf((10, 80, 128), f32), buf((10, 48, 128), f32), buf((7, 48, 128), f32)]
        + [buf((7, 32, 128), f32), buf((5, 32, 128), f32), buf((5, 32, 128), f32)],
        (xa, xb, ea, eb, f2, f3),
        "columns",
        10**8,
        1 << 20,
    )
    ya, yb = swap(ya, "gy", 0), swap(yb, "gy", 1)
    ea, eb, f2, f3, za, zb = call(
        rows_kernel,
        [e, e, f2s, f3s, shape(208, 128), shape(208, 128)],
        [],
        (ya, yb, ea, eb, f2, f3),
        "rows",
        10**8,
        1 << 20,
    )
    za, zb = swap(za, "gz", 0), swap(zb, "gz", 1)
    return tuple(
        call(
            sections_kernel,
            [shape(8, 32, 512), shape(4, 16, 256), shape(2, 8, 128)],
            [],
            (za, zb, ea, eb, f2, f3),
            "sections",
            10**8,
            1 << 20,
        )
    )


def solution(mesh):
    spec = P("gz", "gy", "gx")
    return jax.shard_map(
        on_device, mesh=mesh, in_specs=(spec,), out_specs=(spec,) * 3, check_vma=False
    )
```

```python
import numpy as np
import jax
import jax.numpy as jnp
from jax import lax
from jax.experimental import pallas as pl
from jax.experimental.pallas import tpu as pltpu
from jax.sharding import PartitionSpec as P

taps = (0.0625, 0.25, 0.375, 0.25, 0.0625)
f32, bf16 = jnp.float32, jnp.bfloat16
VMEM = pl.BlockSpec(memory_space=pltpu.VMEM)


def column_weights():
    w = np.zeros((256, 256), np.float32)
    for i in range(-1, 129):
        for k in range(5):
            c = 2 * i - 2 + k
            if 0 <= c < 256:
                lane = i if 0 <= i < 128 else (128 if i == 128 else 255)
                w[c, lane] += taps[k]
    return np.concatenate([w] * 3, axis=0)


def edge_weights():
    w = np.zeros((128, 256), np.float32)
    for c in range(128):
        for k in range(5):
            place = c - 128 if c >= 64 else c
            if (place + 2 - k) % 2:
                continue
            i = (place + 2 - k) // 2
            if c >= 64:
                lane = 128 + i if i < 0 else 128 + i
                w[c, lane] += taps[k]
            else:
                lane = i if i >= 0 else 256 + i
                w[c, lane] += taps[k]
    return np.concatenate([w] * 3, axis=0)


def composite(levels):
    h = np.ones(1)
    for level in range(levels):
        up = np.zeros(4 * 2**level + 1)
        up[:: 2**level] = taps
        h = np.convolve(h, up)
    return h


def shell_weights():
    rows = [(1, 0), (2, 0), (2, 1), (3, 0), (3, 1), (1, -1), (2, -1), (3, -1)]
    w = np.zeros((8, 256), np.float64)
    for r, (level, place) in enumerate(rows):
        h = composite(level)
        reach = len(h) // 2
        for t in range(len(h)):
            c = place * 2**level + t - reach
            if r < 5 and -128 <= c < 0:
                w[r, 256 + c] = h[t]
            if r >= 5 and 0 <= c < 128:
                w[r, c] = h[t]
    high = w.astype(jnp.bfloat16).astype(np.float64)
    return np.concatenate([high, w - high], axis=0).astype(np.float32)


def split(x):
    a = x.astype(bf16)
    r = x - a.astype(f32)
    b = r.astype(bf16)
    return a, b, (r - b.astype(f32)).astype(bf16)


def weigh(p):
    total = None
    for a, b, t in ((p[0], p[4], taps[0]), (p[1], p[3], taps[1]), (p[2], None, taps[2])):
        if a is None and b is None:
            continue
        s = a if b is None else b if a is None else a + b
        total = t * s if total is None else total + t * s
    return total


def keep(axis, count):
    at = lax.axis_index(axis)
    return (
        jnp.where(at > 0, 1.0, 0.0).astype(f32),
        jnp.where(at < count - 1, 1.0, 0.0).astype(f32),
    )


def sections(load, store, first, last, half, above, ends):
    got = {i: load(i) for i in range(first, last + 1)}
    for i in range(-1, half + above):
        v = weigh([got.get(2 * i - 2 + k) for k in range(5)])
        if i < 0:
            v = v * ends[0]
        if i >= half:
            v = v * ends[1]
        store(i, v)


def rows(src, dst, at, half, above, ends):
    n = 2 * half
    dst[at, 8 : 8 + half, :] = weigh(
        [src[at, pl.ds(6 + k, half, stride=2), :] for k in range(5)]
    )
    low = taps[3] * src[at, 7:8, :] + taps[4] * src[at, 8:9, :]
    dst[at, 0:8, :] = jnp.where(
        lax.broadcasted_iota(jnp.int32, (8, 128), 0) == 7, low * ends[0], 0.0
    )
    up = [src[at, 6 + n + k : 7 + n + k, :] for k in range(4)]
    high = weigh(up + [None]) * ends[1]
    higher = (taps[0] * up[2] + taps[1] * up[3]) * ends[1]
    row = lax.broadcasted_iota(jnp.int32, (8, 128), 0)
    dst[at, 8 + half : 16 + half, :] = jnp.where(row == 0, high, jnp.where(row == 1, higher, 0.0))


def pack(parts, dst, at):
    wide = len(parts) * 128
    tall = parts[0].shape[0]
    for j, x in enumerate(parts):
        for q, piece in enumerate(split(x)):
            dst[at : at + tall, q * wide + j * 128 : q * wide + (j + 1) * 128] = piece


def lane():
    return lax.broadcasted_iota(jnp.int32, (8, 128), 1)


def low_lanes(tall):
    return lax.broadcasted_iota(jnp.int32, (tall, 128), 1) < 64


def matmul(x, w):
    return jnp.dot(x, w, preferred_element_type=f32)


def shell_kernel(left, right, w, out):
    x = jnp.concatenate([left[...].reshape(1024, 128), right[...].reshape(1024, 128)], axis=1)
    total = None
    for piece in split(x):
        t = lax.dot_general(w[...], piece, (((1,), (1,)), ((), ())), preferred_element_type=f32)
        total = t if total is None else total + t
    out[...] = total[:8] + total[8:]


def level_one_block(volume, at, zs, ys, ops, res, w, zend, yend):
    for h in range(2):
        cols = pl.ds(at * 256 + h * 128, 128)
        for s in range(10):
            zs[h, s, 0:8, :] = jnp.zeros((8, 128), f32)
            zs[h, s, 72:80, :] = jnp.zeros((8, 128), f32)
        for r in range(0, 64, 8):

            def store(i, v, r=r, h=h):
                zs[h, i + 1, 8 + r : 16 + r, :] = v

            sections(lambda i, r=r, cols=cols: volume[i, r : r + 8, cols], store, 0, 15, 8, 1, zend)
    for s in range(10):
        for h in range(2):
            rows(zs.at[h], ys.at[h], s, 32, 1, yend)
        pack([ys[0, s], ys[1, s]], ops, s * 48)
    res[...] = matmul(ops[...], w[...])


def first_kernel(volume, w, shells, ea, side, again, zs, ys, ops, res):
    again[...] = shells[...]
    zend, yend = keep("gz", lax.axis_size("gz")), keep("gy", lax.axis_size("gy"))
    low = low_lanes(48)
    for b in range(2):
        level_one_block(volume, b, zs, ys, ops, res, w, zend, yend)
        for s in range(10):
            main = res[s * 48 : s * 48 + 48, :128]
            beside = res[s * 48 : s * 48 + 48, 128:]
            if b == 0:
                ea[0, s] = main
                side[s] = beside
            else:
                first = side[s]
                ea[1, s] = main + jnp.where(low, first, 0.0)
                ea[0, s] = ea[0, s] + jnp.where(low, 0.0, beside)
                side[s] = jnp.where(low, beside, first)


def next_level(blocks, edge, zs, ys, ops, edge_ops, res, edge_res, w, we, dst, edge_dst,
               sections_in, half_z, half_y, tall_in, used_in, tall, zend, yend, xend):
    count = len(blocks)
    many = half_z + 3
    for j, src in enumerate(blocks + [edge]):
        for r in range(0, used_in, 8):

            def store(i, v, r=r, j=j):
                zs[j, i + 1, r : r + 8, :] = v

            sections(lambda i, r=r, src=src: src[i + 1, r : r + 8, :], store, -1,
                     sections_in - 2, half_z, 2, zend)
        for s in range(many):
            rows(zs.at[j], ys.at[j], s, half_y, 2, yend)
    size = many * tall
    for p in range(count // 2):
        for s in range(many):
            pack([ys[2 * p, s], ys[2 * p + 1, s]], ops, p * size + s * tall)
    for s in range(many):
        pack([ys[count, s]], edge_ops, s * tall)
    res[...] = matmul(ops[...], w[...])
    edge_res[...] = matmul(edge_ops[...], we[...])
    low = low_lanes(tall)
    last = count // 2 - 1
    for s in range(many):
        mains, besides = [], []
        for p in range(last + 1):
            at = p * size + s * tall
            mains.append(res[at : at + tall, :128])
            besides.append(res[at : at + tall, 128:])
        at = s * tall
        edge_beside = edge_res[at : at + tall, 128:]
        for p in range(last + 1):
            under = besides[p - 1] if p else edge_beside
            over = besides[p + 1] if p < last else edge_beside
            dst[p, s] = mains[p] + jnp.where(low, under, over)
        if edge_dst is not None:
            wrapped = edge_res[at : at + tall, :128] + jnp.where(low, besides[last], besides[0])
            edge_dst[s] = wrapped * jnp.where(low, xend[1], xend[0])


def second_kernel(volume, w, we, ea_in, side, ea, eb, f2, f3,
                  zs, ys, ops, res, h1, z2, y2, ops2, opse2, res2, rese2, h2,
                  z3, y3, ops3, opse3, res3, rese3):
    zend, yend, xend = (keep(a, lax.axis_size(a)) for a in ("gz", "gy", "gx"))
    low = low_lanes(48)
    for b in range(2):
        level_one_block(volume, 2 + b, zs, ys, ops, res, w, zend, yend)
        for s in range(10):
            main = res[s * 48 : s * 48 + 48, :128]
            beside = res[s * 48 : s * 48 + 48, 128:]
            if b == 0:
                eb[0, s] = main + jnp.where(low, side[s], 0.0)
                ea[1, s] = ea[1, s] + jnp.where(low, 0.0, beside)
                h1[s] = beside
            else:
                eb[1, s] = main + jnp.where(low, h1[s], 0.0)
                eb[0, s] = eb[0, s] + jnp.where(low, 0.0, beside)
                h1[s] = jnp.where(low, beside * xend[1], side[s] * xend[0])
    next_level([ea.at[0], ea.at[1], eb.at[0], eb.at[1]], h1, z2, y2, ops2, opse2, res2, rese2,
               w, we, f2, h2, 10, 4, 16, 48, 48, 32, zend, yend, xend)
    next_level([f2.at[0], f2.at[1]], h2, z3, y3, ops3, opse3, res3, rese3,
               w, we, f3, None, 7, 2, 8, 32, 32, 32, zend, yend, xend)


def route(x, base, tall):
    at = lax.broadcasted_iota(jnp.int32, (tall, 128), 1)
    first, count, last = base
    head = x if first == 0 else pltpu.roll(x, 128 - first, axis=1)
    tail = pltpu.roll(x, 127 - last, axis=1)
    return jnp.where(at < count, head, 0.0), jnp.where(at == 127, tail, 0.0)


def columns_kernel(pa, pb, ea_in, eb_in, f2_in, f3_in, ea, eb, f2, f3, ya, yb,
                   flat, zs, y1, z2, y2, z3, y3):
    zend, yend = keep("gz", lax.axis_size("gz")), keep("gy", lax.axis_size("gy"))
    odd = lax.rem(lax.axis_index("gx"), 2) == 1
    row = lax.broadcasted_iota(jnp.int32, (8, 128), 0)
    for j in range(8):
        a, b = pa[:, j * 128 : j * 128 + 128], pb[:, j * 128 : j * 128 + 128]
        under, over = jnp.where(odd, a, b), jnp.where(odd, b, a)
        mine = jnp.where(row < 5, under, over)
        full = jnp.concatenate([mine, jnp.zeros((120, 128), f32)], axis=0)
        flat[2 * j : 2 * j + 2] = full.T.reshape(2, 64, 128)
    for s in range(10):
        zs[s, 0:8, :] = jnp.zeros((8, 128), f32)
        zs[s, 72:80, :] = jnp.zeros((8, 128), f32)
    for r in range(0, 64, 8):

        def store(i, v, r=r):
            zs[i + 1, 8 + r : 16 + r, :] = v

        sections(lambda i, r=r: flat[i, r : r + 8, :], store, 0, 15, 8, 1, zend)
    for s in range(10):
        rows(zs, y1, s, 32, 1, yend)
        head, tail = route(y1[s], (0, 1, 5), 48)
        ea[0, s] = ea[0, s] + head
        eb[1, s] = eb[1, s] + tail
    for r in range(0, 48, 8):

        def store(i, v, r=r):
            z2[i + 1, r : r + 8, :] = v

        sections(lambda i, r=r: y1[i + 1, r : r + 8, :], store, -1, 8, 4, 2, zend)
    for s in range(7):
        rows(z2, y2, s, 16, 2, yend)
        head, tail = route(y2[s], (1, 2, 6), 32)
        f2[0, s] = f2[0, s] + head
        f2[1, s] = f2[1, s] + tail
    for r in range(0, 32, 8):

        def store(i, v, r=r):
            z3[i + 1, r : r + 8, :] = v

        sections(lambda i, r=r: y2[i + 1, r : r + 8, :], store, -1, 5, 2, 2, zend)
    for s in range(5):
        rows(z3, y3, s, 8, 2, yend)
        head, tail = route(y3[s], (3, 2, 7), 32)
        f3[0, s] = f3[0, s] + head + tail

    def emit(dst, high):
        for blk in range(4):
            e = ea if blk < 2 else eb
            for s in range(10):
                at = 40 if high else 7
                dst[blk * 10 + s : blk * 10 + s + 1, :] = e[blk % 2, s, at : at + 1, :]
        for j in range(2 if high else 1):
            for blk in range(2):
                for s in range(7):
                    at, to = 24 + j if high else 7, 40 + j * 14 + blk * 7 + s
                    dst[to : to + 1, :] = f2[blk, s, at : at + 1, :]
            for s in range(5):
                at, to = 16 + j if high else 7, 68 + j * 5 + s
                dst[to : to + 1, :] = f3[0, s, at : at + 1, :]

    odd_row = lax.rem(lax.axis_index("gy"), 2) == 1
    for dst, when in ((ya, odd_row), (yb, jnp.logical_not(odd_row))):
        pl.when(when)(lambda dst=dst: emit(dst, False))
        pl.when(jnp.logical_not(when))(lambda dst=dst: emit(dst, True))


def rows_kernel(pa, pb, ea_in, eb_in, f2_in, f3_in, ea, eb, f2, f3, za, zb):
    odd = lax.rem(lax.axis_index("gy"), 2) == 1
    def got(at):
        a, b = pa[at : at + 1, :], pb[at : at + 1, :]
        return jnp.where(odd, a, b), jnp.where(odd, b, a)

    def add(ref, blk, s, at, v):
        ref[blk, s, at : at + 1, :] = ref[blk, s, at : at + 1, :] + v

    for blk in range(4):
        e = ea if blk < 2 else eb
        for s in range(10):
            under, over = got(blk * 10 + s)
            add(e, blk % 2, s, 8, under)
            add(e, blk % 2, s, 39, over)
    for j in range(2):
        for blk in range(2):
            for s in range(7):
                under, over = got(40 + j * 14 + blk * 7 + s)
                add(f2, blk, s, 8 + j, under)
                if j == 0:
                    add(f2, blk, s, 23, over)
        for s in range(5):
            under, over = got(68 + j * 5 + s)
            add(f3, 0, s, 8 + j, under)
            if j == 0:
                add(f3, 0, s, 15, over)

    def emit(dst, high):
        for blk in range(4):
            e = ea if blk < 2 else eb
            dst[blk * 32 : blk * 32 + 32, :] = e[blk % 2, 9 if high else 0, 8:40, :]
        for j in range(2 if high else 1):
            for blk in range(2):
                to = 128 + j * 32 + blk * 16
                dst[to : to + 16, :] = f2[blk, 5 + j if high else 0, 8:24, :]
            to = 192 + j * 8
            dst[to : to + 8, :] = f3[0, 3 + j if high else 0, 8:16, :]

    odd_slab = lax.rem(lax.axis_index("gz"), 2) == 1
    for dst, when in ((za, odd_slab), (zb, jnp.logical_not(odd_slab))):
        pl.when(when)(lambda dst=dst: emit(dst, False))
        pl.when(jnp.logical_not(when))(lambda dst=dst: emit(dst, True))


def sections_kernel(pa, pb, ea, eb, f2, f3, one, two, three):
    odd = lax.rem(lax.axis_index("gz"), 2) == 1

    def got(at, tall):
        a, b = pa[at : at + tall, :], pb[at : at + tall, :]
        return jnp.where(odd, a, b), jnp.where(odd, b, a)

    for blk in range(4):
        e = ea if blk < 2 else eb
        under, over = got(blk * 32, 32)
        for z in range(8):
            v = e[blk % 2, z + 1, 8:40, :]
            v = v + under if z == 0 else v + over if z == 7 else v
            one[z, :, blk * 128 : blk * 128 + 128] = v
    for blk in range(2):
        under, over = got(128 + blk * 16, 16)
        further, _ = got(160 + blk * 16, 16)
        for z in range(4):
            v = f2[blk, z + 1, 8:24, :]
            v = v + under if z == 0 else v + further if z == 1 else v + over if z == 3 else v
            two[z, :, blk * 128 : blk * 128 + 128] = v
    under, over = got(192, 8)
    further, _ = got(200, 8)
    three[0] = f3[0, 1, 8:16, :] + under
    three[1] = f3[0, 2, 8:16, :] + further + over


def shape(*dims):
    return jax.ShapeDtypeStruct(dims, f32)


def swap(x, axis, first):
    count = lax.axis_size(axis)
    pairs = []
    for i in range(first, count - 1, 2):
        pairs += [(i, i + 1), (i + 1, i)]
    return lax.ppermute(x, axis, pairs)


def call(kernel, outs, scratch, args, name, flops, moved, specs=None, aliases=None, limit=16):
    return pl.pallas_call(
        kernel,
        out_shape=outs,
        in_specs=specs or [VMEM] * len(args),
        out_specs=[VMEM] * len(outs),
        scratch_shapes=scratch,
        input_output_aliases=aliases or {},
        compiler_params=pltpu.CompilerParams(vmem_limit_bytes=limit << 20),
        cost_estimate=pl.CostEstimate(flops=flops, bytes_accessed=moved, transcendentals=0),
        name=name,
    )(*args)


def on_device(volume):
    w = jnp.asarray(column_weights(), bf16)
    we = jnp.asarray(edge_weights(), bf16)
    ws = jnp.asarray(shell_weights(), bf16)
    buf = pltpu.VMEM
    shells = pl.pallas_call(
        shell_kernel,
        grid=(1,),
        out_shape=shape(8, 1024),
        in_specs=[
            pl.BlockSpec((16, 64, 128), lambda i: (0, 0, 0)),
            pl.BlockSpec((16, 64, 128), lambda i: (0, 0, 7)),
            pl.BlockSpec((16, 256), lambda i: (0, 0)),
        ],
        out_specs=pl.BlockSpec((8, 1024), lambda i: (0, 0)),
        compiler_params=pltpu.CompilerParams(vmem_limit_bytes=8 << 20),
        cost_estimate=pl.CostEstimate(flops=10**8, bytes_accessed=1 << 20, transcendentals=0),
        name="shells",
    )(volume, volume, ws)
    xa = swap(shells, "gx", 0)
    block = [buf((2, 10, 80, 128), f32), buf((2, 10, 48, 128), f32), buf((480, 768), bf16), buf((480, 256), f32)]
    e, f2s, f3s = shape(2, 10, 48, 128), shape(2, 7, 32, 128), shape(1, 5, 32, 128)
    ea, side, again = call(
        first_kernel,
        [e, shape(10, 48, 128), shape(8, 1024)],
        block,
        (volume, w, shells),
        "first",
        4 * 10**9,
        1 << 21,
    )
    xb = swap(again, "gx", 1)
    ea, eb, f2, f3 = call(
        second_kernel,
        [e, e, f2s, f3s],
        block
        + [buf((10, 48, 128), f32)]
        + [buf((5, 7, 48, 128), f32), buf((5, 7, 32, 128), f32), buf((448, 768), bf16), buf((224, 384), bf16)]
        + [buf((448, 256), f32), buf((224, 256), f32), buf((7, 32, 128), f32)]
        + [buf((3, 5, 32, 128), f32), buf((3, 5, 32, 128), f32), buf((160, 768), bf16), buf((160, 384), bf16)]
        + [buf((160, 256), f32), buf((160, 256), f32)],
        (volume, w, we, ea, side),
        "second",
        5 * 10**9,
        1 << 21,
        aliases={3: 0},
    )
    keepers = {2: 0, 3: 1, 4: 2, 5: 3}
    ea, eb, f2, f3, ya, yb = call(
        columns_kernel,
        [e, e, f2s, f3s, shape(80, 128), shape(80, 128)],
        [buf((16, 64, 128), f32), buf((10, 80, 128), f32), buf((10, 48, 128), f32), buf((7, 48, 128), f32)]
        + [buf((7, 32, 128), f32), buf((5, 32, 128), f32), buf((5, 32, 128), f32)],
        (xa, xb, ea, eb, f2, f3),
        "columns",
        10**8,
        1 << 20,
        aliases=keepers,
    )
    ya, yb = swap(ya, "gy", 0), swap(yb, "gy", 1)
    ea, eb, f2, f3, za, zb = call(
        rows_kernel,
        [e, e, f2s, f3s, shape(208, 128), shape(208, 128)],
        [],
        (ya, yb, ea, eb, f2, f3),
        "rows",
        10**8,
        1 << 20,
        aliases=keepers,
    )
    za, zb = swap(za, "gz", 0), swap(zb, "gz", 1)
    return tuple(
        call(
            sections_kernel,
            [shape(8, 32, 512), shape(4, 16, 256), shape(2, 8, 128)],
            [],
            (za, zb, ea, eb, f2, f3),
            "sections",
            10**8,
            1 << 20,
        )
    )


def solution(mesh):
    spec = P("gz", "gy", "gx")
    return jax.shard_map(
        on_device, mesh=mesh, in_specs=(spec,), out_specs=(spec,) * 3, check_vma=False
    )
```

```python
import numpy as np
import jax
import jax.numpy as jnp
from jax import lax
from jax.experimental import pallas as pl
from jax.experimental.pallas import tpu as pltpu
from jax.sharding import PartitionSpec as P

taps = (0.0625, 0.25, 0.375, 0.25, 0.0625)
f32, bf16 = jnp.float32, jnp.bfloat16
VMEM = pl.BlockSpec(memory_space=pltpu.VMEM)


def column_weights():
    w = np.zeros((256, 256), np.float32)
    for i in range(-1, 129):
        for k in range(5):
            c = 2 * i - 2 + k
            if 0 <= c < 256:
                lane = i if 0 <= i < 128 else (128 if i == 128 else 255)
                w[c, lane] += taps[k]
    return np.concatenate([w] * 3, axis=0)


def edge_weights():
    w = np.zeros((128, 256), np.float32)
    for c in range(128):
        for k in range(5):
            place = c - 128 if c >= 64 else c
            if (place + 2 - k) % 2:
                continue
            i = (place + 2 - k) // 2
            if c >= 64:
                lane = 128 + i if i < 0 else 128 + i
                w[c, lane] += taps[k]
            else:
                lane = i if i >= 0 else 256 + i
                w[c, lane] += taps[k]
    return np.concatenate([w] * 3, axis=0)


def composite(levels):
    h = np.ones(1)
    for level in range(levels):
        up = np.zeros(4 * 2**level + 1)
        up[:: 2**level] = taps
        h = np.convolve(h, up)
    return h


def shell_weights(first, tall):
    lanes = [(1, 0), (1, -1), (2, 0), (2, 1), (2, -1), (3, 0), (3, 1), (3, -1)]
    c = first + lax.broadcasted_iota(jnp.int32, (tall, 128), 0)
    at = lax.broadcasted_iota(jnp.int32, (tall, 128), 1)
    w = jnp.zeros((tall, 128), f32)
    for r, (level, place) in enumerate(lanes):
        h = composite(level)
        start = place * 2**level - len(h) // 2 + (256 if place >= 0 else 0)
        for t in range(len(h)):
            if first <= start + t < first + tall and (start + t < 256 if place >= 0 else start + t >= 0):
                w = jnp.where((at == r) & (c == start + t), float(h[t]), w)
    high = w.astype(bf16)
    return high, (w - high.astype(f32)).astype(bf16)


def split(x):
    a = x.astype(bf16)
    r = x - a.astype(f32)
    b = r.astype(bf16)
    return a, b, (r - b.astype(f32)).astype(bf16)


def weigh(p):
    total = None
    for a, b, t in ((p[0], p[4], taps[0]), (p[1], p[3], taps[1]), (p[2], None, taps[2])):
        if a is None and b is None:
            continue
        s = a if b is None else b if a is None else a + b
        total = t * s if total is None else total + t * s
    return total


def keep(axis, count):
    at = lax.axis_index(axis)
    return (
        jnp.where(at > 0, 1.0, 0.0).astype(f32),
        jnp.where(at < count - 1, 1.0, 0.0).astype(f32),
    )


def sections(load, store, first, last, half, above, ends):
    got = {i: load(i) for i in range(first, last + 1)}
    for i in range(-1, half + above):
        v = weigh([got.get(2 * i - 2 + k) for k in range(5)])
        if i < 0:
            v = v * ends[0]
        if i >= half:
            v = v * ends[1]
        store(i, v)


def rows(src, dst, at, half, above, ends):
    n = 2 * half
    dst[at, 8 : 8 + half, :] = weigh(
        [src[at, pl.ds(6 + k, half, stride=2), :] for k in range(5)]
    )
    low = taps[3] * src[at, 7:8, :] + taps[4] * src[at, 8:9, :]
    dst[at, 0:8, :] = jnp.where(
        lax.broadcasted_iota(jnp.int32, (8, 128), 0) == 7, low * ends[0], 0.0
    )
    up = [src[at, 6 + n + k : 7 + n + k, :] for k in range(4)]
    high = weigh(up + [None]) * ends[1]
    higher = (taps[0] * up[2] + taps[1] * up[3]) * ends[1]
    row = lax.broadcasted_iota(jnp.int32, (8, 128), 0)
    dst[at, 8 + half : 16 + half, :] = jnp.where(row == 0, high, jnp.where(row == 1, higher, 0.0))


def pack(parts, dst, at):
    wide = len(parts) * 128
    tall = parts[0].shape[0]
    for j, x in enumerate(parts):
        for q, piece in enumerate(split(x)):
            dst[at : at + tall, q * wide + j * 128 : q * wide + (j + 1) * 128] = piece


def lane():
    return lax.broadcasted_iota(jnp.int32, (8, 128), 1)


def low_lanes(tall):
    return lax.broadcasted_iota(jnp.int32, (tall, 128), 1) < 64


def matmul(x, w):
    return jnp.dot(x, w, preferred_element_type=f32)


def pyramid(src, zs, flat, zend, yend):
    z1, z2, z3 = zs
    y1, y2, y3 = (flat.at[pl.ds(o, n * t)].reshape(n, t, 128) for o, n, t in TALL)
    for s in range(10):
        z1[s, 0:8, :] = jnp.zeros((8, 128), f32)
        z1[s, 72:80, :] = jnp.zeros((8, 128), f32)
    for r in range(0, 64, 8):

        def store(i, v, r=r):
            z1[i + 1, 8 + r : 16 + r, :] = v

        sections(lambda i, r=r: src[i, r : r + 8, :], store, 0, 15, 8, 1, zend)
    for s in range(10):
        rows(z1, y1, s, 32, 1, yend)
    for a, zb, b, used, first, half_z, half_y in (
        (y1, z2, y2, 48, 8, 4, 16),
        (y2, z3, y3, 32, 5, 2, 8),
    ):
        for r in range(0, used, 8):

            def store(i, v, r=r, zb=zb):
                zb[i + 1, r : r + 8, :] = v

            sections(lambda i, r=r, a=a: a[i + 1, r : r + 8, :], store, -1, first, half_z, 2, zend)
        for s in range(half_z + 3):
            rows(zb, b, s, half_y, 2, yend)


TALL = ((0, 10, 48), (480, 7, 32), (704, 5, 32))
MIXED = ((3, 96), (5, 64))


def shell_kernel(volume, out, kept, own, w, lines, prod, z1, z2, z3, flat, sems):
    copies = []
    for j, (first, wide) in enumerate(((0, 128), (896, 128), (128, 768))):
        cols = pl.ds(first, wide)
        copies.append(pltpu.make_async_copy(volume.at[:, :, cols], kept.at[:, :, cols], sems.at[j]))
    for c in copies:
        c.start()
    zend, yend = keep("gz", lax.axis_size("gz")), keep("gy", lax.axis_size("gy"))
    w[...] = jnp.zeros((768, 256), bf16)
    for first in (0, 240):
        for j, part in enumerate(shell_weights(first, 16)):
            for q in range(3):
                w[q * 256 + first : q * 256 + first + 16, j * 128 : j * 128 + 128] = part
    for s in range(5):
        flat[704 + s * 32 + 24 : 704 + s * 32 + 32, :] = jnp.zeros((8, 128), f32)
    flat[864:896, :] = jnp.zeros((32, 128), f32)
    out[16:24, :] = jnp.zeros((8, 128), f32)
    copies[0].wait()
    copies[1].wait()
    for s in range(16):
        pack([kept[s, :, 0:128], kept[s, :, 896:1024]], lines, s * 64)
    prod[...] = matmul(lines[...], w[...])
    for s in range(16):
        lines_s = prod[s * 64 : s * 64 + 64, :]
        own[s] = lines_s[:, :128] + lines_s[:, 128:]
    pyramid(own, (z1, z2, z3), flat, zend, yend)
    at = lax.broadcasted_iota(jnp.int32, (1, 128), 1)
    mixed = dict(MIXED)
    for j in range(7):
        t = flat[j * 128 : j * 128 + 128, :].T
        pick = [(t[0:1], None, t[1:2]), (t[2:3], t[3:4], t[4:5]), (t[5:6], t[6:7], t[7:8])]
        level = 0 if j < 4 else 1 if j < 6 else 2
        for q in range(3):
            row = pick[level][q]
            row = jnp.zeros((1, 128), f32) if row is None else row
            if j in mixed:
                row = jnp.where(at < mixed[j], row, pick[level + 1][q])
            out[3 * j + q : 3 * j + q + 1, :] = row
    copies[2].wait()


def level_one_block(volume, at, zs, ys, ops, res, w, zend, yend):
    for h in range(2):
        cols = pl.ds(at * 256 + h * 128, 128)
        for s in range(10):
            zs[h, s, 0:8, :] = jnp.zeros((8, 128), f32)
            zs[h, s, 72:80, :] = jnp.zeros((8, 128), f32)
        for r in range(0, 64, 8):

            def store(i, v, r=r, h=h):
                zs[h, i + 1, 8 + r : 16 + r, :] = v

            sections(lambda i, r=r, cols=cols: volume[i, r : r + 8, cols], store, 0, 15, 8, 1, zend)
    for s in range(10):
        for h in range(2):
            rows(zs.at[h], ys.at[h], s, 32, 1, yend)
        pack([ys[0, s], ys[1, s]], ops, s * 48)
    res[...] = matmul(ops[...], w[...])


def first_kernel(volume, w, shells, ea, side, again, zs, ys, ops, res):
    again[...] = shells[...]
    zend, yend = keep("gz", lax.axis_size("gz")), keep("gy", lax.axis_size("gy"))
    low = low_lanes(48)
    for b in range(2):
        level_one_block(volume, b, zs, ys, ops, res, w, zend, yend)
        for s in range(10):
            main = res[s * 48 : s * 48 + 48, :128]
            beside = res[s * 48 : s * 48 + 48, 128:]
            if b == 0:
                ea[0, s] = main
                side[s] = beside
            else:
                first = side[s]
                ea[1, s] = main + jnp.where(low, first, 0.0)
                ea[0, s] = ea[0, s] + jnp.where(low, 0.0, beside)
                side[s] = jnp.where(low, beside, first)


def next_level(blocks, edge, zs, ys, ops, edge_ops, res, edge_res, w, we, dst, edge_dst,
               sections_in, half_z, half_y, tall_in, used_in, tall, zend, yend, xend):
    count = len(blocks)
    many = half_z + 3
    for j, src in enumerate(blocks + [edge]):
        for r in range(0, used_in, 8):

            def store(i, v, r=r, j=j):
                zs[j, i + 1, r : r + 8, :] = v

            sections(lambda i, r=r, src=src: src[i + 1, r : r + 8, :], store, -1,
                     sections_in - 2, half_z, 2, zend)
        for s in range(many):
            rows(zs.at[j], ys.at[j], s, half_y, 2, yend)
    size = many * tall
    for p in range(count // 2):
        for s in range(many):
            pack([ys[2 * p, s], ys[2 * p + 1, s]], ops, p * size + s * tall)
    for s in range(many):
        pack([ys[count, s]], edge_ops, s * tall)
    res[...] = matmul(ops[...], w[...])
    edge_res[...] = matmul(edge_ops[...], we[...])
    low = low_lanes(tall)
    last = count // 2 - 1
    for s in range(many):
        mains, besides = [], []
        for p in range(last + 1):
            at = p * size + s * tall
            mains.append(res[at : at + tall, :128])
            besides.append(res[at : at + tall, 128:])
        at = s * tall
        edge_beside = edge_res[at : at + tall, 128:]
        for p in range(last + 1):
            under = besides[p - 1] if p else edge_beside
            over = besides[p + 1] if p < last else edge_beside
            dst[p, s] = mains[p] + jnp.where(low, under, over)
        if edge_dst is not None:
            wrapped = edge_res[at : at + tall, :128] + jnp.where(low, besides[last], besides[0])
            edge_dst[s] = wrapped * jnp.where(low, xend[1], xend[0])


def second_kernel(volume, w, we, ea_in, side, ea, eb, f2, f3,
                  zs, ys, ops, res, h1, z2, y2, ops2, opse2, res2, rese2, h2,
                  z3, y3, ops3, opse3, res3, rese3):
    zend, yend, xend = (keep(a, lax.axis_size(a)) for a in ("gz", "gy", "gx"))
    low = low_lanes(48)
    for b in range(2):
        level_one_block(volume, 2 + b, zs, ys, ops, res, w, zend, yend)
        for s in range(10):
            main = res[s * 48 : s * 48 + 48, :128]
            beside = res[s * 48 : s * 48 + 48, 128:]
            if b == 0:
                eb[0, s] = main + jnp.where(low, side[s], 0.0)
                ea[1, s] = ea[1, s] + jnp.where(low, 0.0, beside)
                h1[s] = beside
            else:
                eb[1, s] = main + jnp.where(low, h1[s], 0.0)
                eb[0, s] = eb[0, s] + jnp.where(low, 0.0, beside)
                h1[s] = jnp.where(low, beside * xend[1], side[s] * xend[0])
    next_level([ea.at[0], ea.at[1], eb.at[0], eb.at[1]], h1, z2, y2, ops2, opse2, res2, rese2,
               w, we, f2, h2, 10, 4, 16, 48, 48, 32, zend, yend, xend)
    next_level([f2.at[0], f2.at[1]], h2, z3, y3, ops3, opse3, res3, rese3,
               w, we, f3, None, 7, 2, 8, 32, 32, 32, zend, yend, xend)


def columns_kernel(pa, pb, ea_in, eb_in, f2_in, f3_in, ea, eb, f2, f3, ya, yb, flat):
    odd = lax.rem(lax.axis_index("gx"), 2) == 1
    for j in range(7):
        a, b = pa[3 * j : 3 * j + 3, :], pb[3 * j : 3 * j + 3, :]
        under, over = jnp.where(odd, a, b), jnp.where(odd, b, a)
        full = jnp.concatenate([under[:2], jnp.zeros((125, 128), f32), over[2:]], axis=0)
        flat[j * 128 : j * 128 + 128, :] = full.T
    low = low_lanes(48)
    for s in range(10):
        v = flat[s * 48 : s * 48 + 48, :]
        ea[0, s] = ea[0, s] + jnp.where(low, v, 0.0)
        eb[1, s] = eb[1, s] + jnp.where(low, 0.0, v)
    low = low_lanes(32)
    for s in range(7):
        v = flat[480 + s * 32 : 512 + s * 32, :]
        f2[0, s] = f2[0, s] + jnp.where(low, v, 0.0)
        f2[1, s] = f2[1, s] + jnp.where(low, 0.0, v)
    for s in range(5):
        f3[0, s] = f3[0, s] + flat[704 + s * 32 : 736 + s * 32, :]

    def emit(dst, high):
        for blk in range(4):
            e = ea if blk < 2 else eb
            for s in range(10):
                at = 40 if high else 7
                dst[blk * 10 + s : blk * 10 + s + 1, :] = e[blk % 2, s, at : at + 1, :]
        for j in range(2 if high else 1):
            for blk in range(2):
                for s in range(7):
                    at, to = 24 + j if high else 7, 40 + j * 14 + blk * 7 + s
                    dst[to : to + 1, :] = f2[blk, s, at : at + 1, :]
            for s in range(5):
                at, to = 16 + j if high else 7, 68 + j * 5 + s
                dst[to : to + 1, :] = f3[0, s, at : at + 1, :]

    odd_row = lax.rem(lax.axis_index("gy"), 2) == 1
    for dst, when in ((ya, odd_row), (yb, jnp.logical_not(odd_row))):
        pl.when(when)(lambda dst=dst: emit(dst, False))
        pl.when(jnp.logical_not(when))(lambda dst=dst: emit(dst, True))


def rows_kernel(pa, pb, ea_in, eb_in, f2_in, f3_in, ea, eb, f2, f3, za, zb):
    odd = lax.rem(lax.axis_index("gy"), 2) == 1
    def got(at):
        a, b = pa[at : at + 1, :], pb[at : at + 1, :]
        return jnp.where(odd, a, b), jnp.where(odd, b, a)

    def add(ref, blk, s, at, v):
        ref[blk, s, at : at + 1, :] = ref[blk, s, at : at + 1, :] + v

    for blk in range(4):
        e = ea if blk < 2 else eb
        for s in range(10):
            under, over = got(blk * 10 + s)
            add(e, blk % 2, s, 8, under)
            add(e, blk % 2, s, 39, over)
    for j in range(2):
        for blk in range(2):
            for s in range(7):
                under, over = got(40 + j * 14 + blk * 7 + s)
                add(f2, blk, s, 8 + j, under)
                if j == 0:
                    add(f2, blk, s, 23, over)
        for s in range(5):
            under, over = got(68 + j * 5 + s)
            add(f3, 0, s, 8 + j, under)
            if j == 0:
                add(f3, 0, s, 15, over)

    def emit(dst, high):
        for blk in range(4):
            e = ea if blk < 2 else eb
            dst[blk * 32 : blk * 32 + 32, :] = e[blk % 2, 9 if high else 0, 8:40, :]
        for j in range(2 if high else 1):
            for blk in range(2):
                to = 128 + j * 32 + blk * 16
                dst[to : to + 16, :] = f2[blk, 5 + j if high else 0, 8:24, :]
            to = 192 + j * 8
            dst[to : to + 8, :] = f3[0, 3 + j if high else 0, 8:16, :]

    odd_slab = lax.rem(lax.axis_index("gz"), 2) == 1
    for dst, when in ((za, odd_slab), (zb, jnp.logical_not(odd_slab))):
        pl.when(when)(lambda dst=dst: emit(dst, False))
        pl.when(jnp.logical_not(when))(lambda dst=dst: emit(dst, True))


def sections_kernel(pa, pb, ea, eb, f2, f3, one, two, three):
    odd = lax.rem(lax.axis_index("gz"), 2) == 1

    def got(at, tall):
        a, b = pa[at : at + tall, :], pb[at : at + tall, :]
        return jnp.where(odd, a, b), jnp.where(odd, b, a)

    for blk in range(4):
        e = ea if blk < 2 else eb
        under, over = got(blk * 32, 32)
        for z in range(8):
            v = e[blk % 2, z + 1, 8:40, :]
            v = v + under if z == 0 else v + over if z == 7 else v
            one[z, :, blk * 128 : blk * 128 + 128] = v
    for blk in range(2):
        under, over = got(128 + blk * 16, 16)
        further, _ = got(160 + blk * 16, 16)
        for z in range(4):
            v = f2[blk, z + 1, 8:24, :]
            v = v + under if z == 0 else v + further if z == 1 else v + over if z == 3 else v
            two[z, :, blk * 128 : blk * 128 + 128] = v
    under, over = got(192, 8)
    further, _ = got(200, 8)
    three[0] = f3[0, 1, 8:16, :] + under
    three[1] = f3[0, 2, 8:16, :] + further + over


def shape(*dims):
    return jax.ShapeDtypeStruct(dims, f32)


def swap(x, axis, first):
    count = lax.axis_size(axis)
    pairs = []
    for i in range(first, count - 1, 2):
        pairs += [(i, i + 1), (i + 1, i)]
    return lax.ppermute(x, axis, pairs)


def call(kernel, outs, scratch, args, name, flops, moved, specs=None, aliases=None, limit=16):
    return pl.pallas_call(
        kernel,
        out_shape=outs,
        in_specs=specs or [VMEM] * len(args),
        out_specs=[VMEM] * len(outs),
        scratch_shapes=scratch,
        input_output_aliases=aliases or {},
        compiler_params=pltpu.CompilerParams(vmem_limit_bytes=limit << 20),
        cost_estimate=pl.CostEstimate(flops=flops, bytes_accessed=moved, transcendentals=0),
        name=name,
    )(*args)


def on_device(volume):
    w = jnp.asarray(column_weights(), bf16)
    we = jnp.asarray(edge_weights(), bf16)
    buf = pltpu.VMEM
    levels = [buf((10, 80, 128), f32), buf((7, 48, 128), f32), buf((5, 32, 128), f32)]
    shells, volume = call(
        shell_kernel,
        [shape(24, 128), shape(16, 64, 1024)],
        [buf((16, 64, 128), f32)]
        + [buf((768, 256), bf16), buf((1024, 768), bf16), buf((1024, 256), f32)]
        + levels
        + [buf((896, 128), f32), pltpu.SemaphoreType.DMA((3,))],
        (volume,),
        "shells",
        10**8,
        1 << 20,
        specs=[pl.BlockSpec(memory_space=pltpu.HBM)],
        limit=48,
    )
    xa = swap(shells, "gx", 0)
    block = [buf((2, 10, 80, 128), f32), buf((2, 10, 48, 128), f32), buf((480, 768), bf16), buf((480, 256), f32)]
    e, f2s, f3s = shape(2, 10, 48, 128), shape(2, 7, 32, 128), shape(1, 5, 32, 128)
    ea, side, again = call(
        first_kernel,
        [e, shape(10, 48, 128), shape(24, 128)],
        block,
        (volume, w, shells),
        "first",
        4 * 10**9,
        1 << 21,
    )
    xb = swap(again, "gx", 1)
    ea, eb, f2, f3 = call(
        second_kernel,
        [e, e, f2s, f3s],
        block
        + [buf((10, 48, 128), f32)]
        + [buf((5, 7, 48, 128), f32), buf((5, 7, 32, 128), f32), buf((448, 768), bf16), buf((224, 384), bf16)]
        + [buf((448, 256), f32), buf((224, 256), f32), buf((7, 32, 128), f32)]
        + [buf((3, 5, 32, 128), f32), buf((3, 5, 32, 128), f32), buf((160, 768), bf16), buf((160, 384), bf16)]
        + [buf((160, 256), f32), buf((160, 256), f32)],
        (volume, w, we, ea, side),
        "second",
        5 * 10**9,
        1 << 21,
        aliases={3: 0},
    )
    keepers = {2: 0, 3: 1, 4: 2, 5: 3}
    ea, eb, f2, f3, ya, yb = call(
        columns_kernel,
        [e, e, f2s, f3s, shape(80, 128), shape(80, 128)],
        [buf((896, 128), f32)],
        (xa, xb, ea, eb, f2, f3),
        "columns",
        10**8,
        1 << 20,
        aliases=keepers,
    )
    ya, yb = swap(ya, "gy", 0), swap(yb, "gy", 1)
    ea, eb, f2, f3, za, zb = call(
        rows_kernel,
        [e, e, f2s, f3s, shape(208, 128), shape(208, 128)],
        [],
        (ya, yb, ea, eb, f2, f3),
        "rows",
        10**8,
        1 << 20,
        aliases=keepers,
    )
    za, zb = swap(za, "gz", 0), swap(zb, "gz", 1)
    return tuple(
        call(
            sections_kernel,
            [shape(8, 32, 512), shape(4, 16, 256), shape(2, 8, 128)],
            [],
            (za, zb, ea, eb, f2, f3),
            "sections",
            10**8,
            1 << 20,
        )
    )


def solution(mesh):
    spec = P("gz", "gy", "gx")
    return jax.shard_map(
        on_device, mesh=mesh, in_specs=(spec,), out_specs=(spec,) * 3, check_vma=False
    )
```

```python
import numpy as np
import jax
import jax.numpy as jnp
from jax import lax
from jax.experimental import pallas as pl
from jax.experimental.pallas import tpu as pltpu
from jax.sharding import PartitionSpec as P


taps = (0.0625, 0.25, 0.375, 0.25, 0.0625)
f32, bf16 = jnp.float32, jnp.bfloat16
VMEM = pl.BlockSpec(memory_space=pltpu.VMEM)


def column_weights():
    w = np.zeros((256, 256), np.float32)
    for i in range(-1, 129):
        for k in range(5):
            c = 2 * i - 2 + k
            if 0 <= c < 256:
                lane = i if 0 <= i < 128 else (128 if i == 128 else 255)
                w[c, lane] += taps[k]
    return np.concatenate([w] * 3, axis=0)


def edge_weights():
    w = np.zeros((128, 256), np.float32)
    for c in range(128):
        for k in range(5):
            place = c - 128 if c >= 64 else c
            if (place + 2 - k) % 2:
                continue
            i = (place + 2 - k) // 2
            if c >= 64:
                lane = 128 + i
                w[c, lane] += taps[k]
            else:
                lane = i if i >= 0 else 256 + i
                w[c, lane] += taps[k]
    return np.concatenate([w] * 3, axis=0)


def composite(levels):
    h = np.ones(1)
    for level in range(levels):
        up = np.zeros(4 * 2**level + 1)
        up[:: 2**level] = taps
        h = np.convolve(h, up)
    return h


def shell_weights(first, tall):
    lanes = [(1, 0), (1, -1), (2, 0), (2, 1), (2, -1), (3, 0), (3, 1), (3, -1)]
    c = first + lax.broadcasted_iota(jnp.int32, (tall, 128), 0)
    at = lax.broadcasted_iota(jnp.int32, (tall, 128), 1)
    w = jnp.zeros((tall, 128), f32)
    for r, (level, place) in enumerate(lanes):
        h = composite(level)
        start = place * 2**level - len(h) // 2 + (256 if place >= 0 else 0)
        for t in range(len(h)):
            if first <= start + t < first + tall and (start + t < 256 if place >= 0 else start + t >= 0):
                w = jnp.where((at == r) & (c == start + t), float(h[t]), w)
    high = w.astype(bf16)
    return high, (w - high.astype(f32)).astype(bf16)


def split(x):
    a = x.astype(bf16)
    r = x - a.astype(f32)
    b = r.astype(bf16)
    return a, b, (r - b.astype(f32)).astype(bf16)


def weigh(p):
    total = None
    for a, b, t in ((p[0], p[4], taps[0]), (p[1], p[3], taps[1]), (p[2], None, taps[2])):
        if a is None and b is None:
            continue
        s = a if b is None else b if a is None else a + b
        total = t * s if total is None else total + t * s
    return total


def keep(axis, count):
    at = lax.axis_index(axis)
    return (
        jnp.where(at > 0, 1.0, 0.0).astype(f32),
        jnp.where(at < count - 1, 1.0, 0.0).astype(f32),
    )


def sections(load, store, first, last, half, above, ends):
    got = {i: load(i) for i in range(first, last + 1)}
    for i in range(-1, half + above):
        v = weigh([got.get(2 * i - 2 + k) for k in range(5)])
        if i < 0:
            v = v * ends[0]
        if i >= half:
            v = v * ends[1]
        store(i, v)


def rows(src, dst, at, half, ends):
    n = 2 * half
    dst[at, 8 : 8 + half, :] = weigh(
        [src[at, pl.ds(6 + k, half, stride=2), :] for k in range(5)]
    )
    low = taps[3] * src[at, 7:8, :] + taps[4] * src[at, 8:9, :]
    dst[at, 0:8, :] = jnp.where(
        lax.broadcasted_iota(jnp.int32, (8, 128), 0) == 7, low * ends[0], 0.0
    )
    up = [src[at, 6 + n + k : 7 + n + k, :] for k in range(4)]
    high = weigh(up + [None]) * ends[1]
    higher = (taps[0] * up[2] + taps[1] * up[3]) * ends[1]
    row = lax.broadcasted_iota(jnp.int32, (8, 128), 0)
    dst[at, 8 + half : 16 + half, :] = jnp.where(row == 0, high, jnp.where(row == 1, higher, 0.0))


def pack(parts, dst, at):
    wide = len(parts) * 128
    tall = parts[0].shape[0]
    for j, x in enumerate(parts):
        for q, piece in enumerate(split(x)):
            dst[at : at + tall, q * wide + j * 128 : q * wide + (j + 1) * 128] = piece


def low_lanes(tall):
    return lax.broadcasted_iota(jnp.int32, (tall, 128), 1) < 64


def matmul(x, w):
    return jnp.dot(x, w, preferred_element_type=f32)


def pyramid(src, zs, flat, zend, yend):
    z1, z2, z3 = zs
    y1, y2, y3 = (flat.at[pl.ds(o, n * t)].reshape(n, t, 128) for o, n, t in TALL)
    for s in range(10):
        z1[s, 0:8, :] = jnp.zeros((8, 128), f32)
        z1[s, 72:80, :] = jnp.zeros((8, 128), f32)
    for r in range(0, 64, 8):

        def store(i, v, r=r):
            z1[i + 1, 8 + r : 16 + r, :] = v

        sections(lambda i, r=r: src[i, r : r + 8, :], store, 0, 15, 8, 1, zend)
    for s in range(10):
        rows(z1, y1, s, 32, yend)
    for a, zb, b, used, first, half_z, half_y in (
        (y1, z2, y2, 48, 8, 4, 16),
        (y2, z3, y3, 32, 5, 2, 8),
    ):
        for r in range(0, used, 8):

            def store(i, v, r=r, zb=zb):
                zb[i + 1, r : r + 8, :] = v

            sections(lambda i, r=r, a=a: a[i + 1, r : r + 8, :], store, -1, first, half_z, 2, zend)
        for s in range(half_z + 3):
            rows(zb, b, s, half_y, yend)


TALL = ((0, 10, 48), (480, 7, 32), (704, 5, 32))
MIXED = ((3, 96), (5, 64))


def shell_kernel(volume, out, kept, own, w, lines, prod, z1, z2, z3, flat, sems):
    copies = []
    for j, (first, wide) in enumerate(((0, 128), (896, 128), (128, 768))):
        cols = pl.ds(first, wide)
        copies.append(pltpu.make_async_copy(volume.at[:, :, cols], kept.at[:, :, cols], sems.at[j]))
    for c in copies:
        c.start()
    zend, yend = keep("gz", lax.axis_size("gz")), keep("gy", lax.axis_size("gy"))
    w[...] = jnp.zeros((768, 256), bf16)
    for first in (0, 240):
        for j, part in enumerate(shell_weights(first, 16)):
            for q in range(3):
                w[q * 256 + first : q * 256 + first + 16, j * 128 : j * 128 + 128] = part
    for s in range(5):
        flat[704 + s * 32 + 24 : 704 + s * 32 + 32, :] = jnp.zeros((8, 128), f32)
    flat[864:896, :] = jnp.zeros((32, 128), f32)
    out[16:24, :] = jnp.zeros((8, 128), f32)
    copies[0].wait()
    copies[1].wait()
    for s in range(16):
        pack([kept[s, :, 0:128], kept[s, :, 896:1024]], lines, s * 64)
    prod[...] = matmul(lines[...], w[...])
    for s in range(16):
        lines_s = prod[s * 64 : s * 64 + 64, :]
        own[s] = lines_s[:, :128] + lines_s[:, 128:]
    pyramid(own, (z1, z2, z3), flat, zend, yend)
    at = lax.broadcasted_iota(jnp.int32, (1, 128), 1)
    mixed = dict(MIXED)
    for j in range(7):
        t = flat[j * 128 : j * 128 + 128, :].T
        pick = [(t[0:1], None, t[1:2]), (t[2:3], t[3:4], t[4:5]), (t[5:6], t[6:7], t[7:8])]
        level = 0 if j < 4 else 1 if j < 6 else 2
        for q in range(3):
            row = pick[level][q]
            row = jnp.zeros((1, 128), f32) if row is None else row
            if j in mixed:
                row = jnp.where(at < mixed[j], row, pick[level + 1][q])
            out[3 * j + q : 3 * j + q + 1, :] = row
    copies[2].wait()


def level_one_block(volume, at, zs, ys, ops, res, w, zend, yend):
    for h in range(2):
        cols = pl.ds(at * 256 + h * 128, 128)
        for s in range(10):
            zs[h, s, 0:8, :] = jnp.zeros((8, 128), f32)
            zs[h, s, 72:80, :] = jnp.zeros((8, 128), f32)
        for r in range(0, 64, 8):

            def store(i, v, r=r, h=h):
                zs[h, i + 1, 8 + r : 16 + r, :] = v

            sections(lambda i, r=r, cols=cols: volume[i, r : r + 8, cols], store, 0, 15, 8, 1, zend)
    for s in range(10):
        for h in range(2):
            rows(zs.at[h], ys.at[h], s, 32, yend)
        pack([ys[0, s], ys[1, s]], ops, s * 48)
    res[...] = matmul(ops[...], w[...])


def first_half(volume, w, ea, side, zs, ys, ops, res, zend, yend):
    low = low_lanes(48)
    for b in range(2):
        level_one_block(volume, b, zs, ys, ops, res, w, zend, yend)
        for s in range(10):
            main = res[s * 48 : s * 48 + 48, :128]
            beside = res[s * 48 : s * 48 + 48, 128:]
            if b == 0:
                ea[0, s] = main
                side[s] = beside
            else:
                first = side[s]
                ea[1, s] = main + jnp.where(low, first, 0.0)
                ea[0, s] = ea[0, s] + jnp.where(low, 0.0, beside)
                side[s] = jnp.where(low, beside, first)


def early():
    return lax.axis_index("gx") < lax.axis_size("gx") // 2


def first_kernel(volume, w, shells, ea, side, again, zs, ys, ops, res):
    again[...] = shells[...]
    zend, yend = keep("gz", lax.axis_size("gz")), keep("gy", lax.axis_size("gy"))

    @pl.when(early())
    def _():
        first_half(volume, w, ea, side, zs, ys, ops, res, zend, yend)


def next_level(blocks, edge, zs, ys, ops, edge_ops, res, edge_res, w, we, dst, edge_dst,
               sections_in, half_z, half_y, used_in, tall, zend, yend, xend):
    count = len(blocks)
    many = half_z + 3
    for j, src in enumerate(blocks + [edge]):
        for r in range(0, used_in, 8):

            def store(i, v, r=r, j=j):
                zs[j, i + 1, r : r + 8, :] = v

            sections(lambda i, r=r, src=src: src[i + 1, r : r + 8, :], store, -1,
                     sections_in - 2, half_z, 2, zend)
        for s in range(many):
            rows(zs.at[j], ys.at[j], s, half_y, yend)
    size = many * tall
    for p in range(count // 2):
        for s in range(many):
            pack([ys[2 * p, s], ys[2 * p + 1, s]], ops, p * size + s * tall)
    for s in range(many):
        pack([ys[count, s]], edge_ops, s * tall)
    res[...] = matmul(ops[...], w[...])
    edge_res[...] = matmul(edge_ops[...], we[...])
    low = low_lanes(tall)
    last = count // 2 - 1
    for s in range(many):
        mains, besides = [], []
        for p in range(last + 1):
            at = p * size + s * tall
            mains.append(res[at : at + tall, :128])
            besides.append(res[at : at + tall, 128:])
        at = s * tall
        edge_beside = edge_res[at : at + tall, 128:]
        for p in range(last + 1):
            under = besides[p - 1] if p else edge_beside
            over = besides[p + 1] if p < last else edge_beside
            dst[p, s] = mains[p] + jnp.where(low, under, over)
        if edge_dst is not None:
            wrapped = edge_res[at : at + tall, :128] + jnp.where(low, besides[last], besides[0])
            edge_dst[s] = wrapped * jnp.where(low, xend[1], xend[0])


def second_kernel(volume, w, we, ea_in, side_in, ea, side, eb, f2, f3,
                  zs, ys, ops, res, h1, z2, y2, ops2, opse2, res2, rese2, h2,
                  z3, y3, ops3, opse3, res3, rese3):
    zend, yend, xend = (keep(a, lax.axis_size(a)) for a in ("gz", "gy", "gx"))
    low = low_lanes(48)

    @pl.when(jnp.logical_not(early()))
    def _():
        first_half(volume, w, ea, side, zs, ys, ops, res, zend, yend)

    for b in range(2):
        level_one_block(volume, 2 + b, zs, ys, ops, res, w, zend, yend)
        for s in range(10):
            main = res[s * 48 : s * 48 + 48, :128]
            beside = res[s * 48 : s * 48 + 48, 128:]
            if b == 0:
                eb[0, s] = main + jnp.where(low, side[s], 0.0)
                ea[1, s] = ea[1, s] + jnp.where(low, 0.0, beside)
                h1[s] = beside
            else:
                eb[1, s] = main + jnp.where(low, h1[s], 0.0)
                eb[0, s] = eb[0, s] + jnp.where(low, 0.0, beside)
                h1[s] = jnp.where(low, beside * xend[1], side[s] * xend[0])
    next_level([ea.at[0], ea.at[1], eb.at[0], eb.at[1]], h1, z2, y2, ops2, opse2, res2, rese2,
               w, we, f2, h2, 10, 4, 16, 48, 32, zend, yend, xend)
    next_level([f2.at[0], f2.at[1]], h2, z3, y3, ops3, opse3, res3, rese3,
               w, we, f3, None, 7, 2, 8, 32, 32, zend, yend, xend)


def columns_kernel(pa, pb, ea_in, eb_in, f2_in, f3_in, ea, eb, f2, f3, ya, yb, flat):
    odd = lax.rem(lax.axis_index("gx"), 2) == 1
    for j in range(7):
        a, b = pa[3 * j : 3 * j + 3, :], pb[3 * j : 3 * j + 3, :]
        under, over = jnp.where(odd, a, b), jnp.where(odd, b, a)
        full = jnp.concatenate([under[:2], jnp.zeros((125, 128), f32), over[2:]], axis=0)
        flat[j * 128 : j * 128 + 128, :] = full.T
    low = low_lanes(48)
    for s in range(10):
        v = flat[s * 48 : s * 48 + 48, :]
        ea[0, s] = ea[0, s] + jnp.where(low, v, 0.0)
        eb[1, s] = eb[1, s] + jnp.where(low, 0.0, v)
    low = low_lanes(32)
    for s in range(7):
        v = flat[480 + s * 32 : 512 + s * 32, :]
        f2[0, s] = f2[0, s] + jnp.where(low, v, 0.0)
        f2[1, s] = f2[1, s] + jnp.where(low, 0.0, v)
    for s in range(5):
        f3[0, s] = f3[0, s] + flat[704 + s * 32 : 736 + s * 32, :]

    def emit(dst, high):
        for blk in range(4):
            e = ea if blk < 2 else eb
            for s in range(10):
                at = 40 if high else 7
                dst[blk * 10 + s : blk * 10 + s + 1, :] = e[blk % 2, s, at : at + 1, :]
        for j in range(2 if high else 1):
            for blk in range(2):
                for s in range(7):
                    at, to = 24 + j if high else 7, 40 + j * 14 + blk * 7 + s
                    dst[to : to + 1, :] = f2[blk, s, at : at + 1, :]
            for s in range(5):
                at, to = 16 + j if high else 7, 68 + j * 5 + s
                dst[to : to + 1, :] = f3[0, s, at : at + 1, :]

    odd_row = lax.rem(lax.axis_index("gy"), 2) == 1
    for dst, when in ((ya, odd_row), (yb, jnp.logical_not(odd_row))):
        pl.when(when)(lambda dst=dst: emit(dst, False))
        pl.when(jnp.logical_not(when))(lambda dst=dst: emit(dst, True))


def rows_kernel(pa, pb, ea_in, eb_in, f2_in, f3_in, ea, eb, f2, f3, za, zb):
    odd = lax.rem(lax.axis_index("gy"), 2) == 1

    def got(at):
        a, b = pa[at : at + 1, :], pb[at : at + 1, :]
        return jnp.where(odd, a, b), jnp.where(odd, b, a)

    def add(ref, blk, s, at, v):
        ref[blk, s, at : at + 1, :] = ref[blk, s, at : at + 1, :] + v

    for blk in range(4):
        e = ea if blk < 2 else eb
        for s in range(10):
            under, over = got(blk * 10 + s)
            add(e, blk % 2, s, 8, under)
            add(e, blk % 2, s, 39, over)
    for j in range(2):
        for blk in range(2):
            for s in range(7):
                under, over = got(40 + j * 14 + blk * 7 + s)
                add(f2, blk, s, 8 + j, under)
                if j == 0:
                    add(f2, blk, s, 23, over)
        for s in range(5):
            under, over = got(68 + j * 5 + s)
            add(f3, 0, s, 8 + j, under)
            if j == 0:
                add(f3, 0, s, 15, over)

    def emit(dst, high):
        for blk in range(4):
            e = ea if blk < 2 else eb
            dst[blk * 32 : blk * 32 + 32, :] = e[blk % 2, 9 if high else 0, 8:40, :]
        for j in range(2 if high else 1):
            for blk in range(2):
                to = 128 + j * 32 + blk * 16
                dst[to : to + 16, :] = f2[blk, 5 + j if high else 0, 8:24, :]
            to = 192 + j * 8
            dst[to : to + 8, :] = f3[0, 3 + j if high else 0, 8:16, :]

    odd_slab = lax.rem(lax.axis_index("gz"), 2) == 1
    for dst, when in ((za, odd_slab), (zb, jnp.logical_not(odd_slab))):
        pl.when(when)(lambda dst=dst: emit(dst, False))
        pl.when(jnp.logical_not(when))(lambda dst=dst: emit(dst, True))


def sections_kernel(pa, pb, ea, eb, f2, f3, one, two, three):
    odd = lax.rem(lax.axis_index("gz"), 2) == 1

    def got(at, tall):
        a, b = pa[at : at + tall, :], pb[at : at + tall, :]
        return jnp.where(odd, a, b), jnp.where(odd, b, a)

    for blk in range(4):
        e = ea if blk < 2 else eb
        under, over = got(blk * 32, 32)
        for z in range(8):
            v = e[blk % 2, z + 1, 8:40, :]
            v = v + under if z == 0 else v + over if z == 7 else v
            one[z, :, blk * 128 : blk * 128 + 128] = v
    for blk in range(2):
        under, over = got(128 + blk * 16, 16)
        further, _ = got(160 + blk * 16, 16)
        for z in range(4):
            v = f2[blk, z + 1, 8:24, :]
            v = v + under if z == 0 else v + further if z == 1 else v + over if z == 3 else v
            two[z, :, blk * 128 : blk * 128 + 128] = v
    under, over = got(192, 8)
    further, _ = got(200, 8)
    three[0] = f3[0, 1, 8:16, :] + under
    three[1] = f3[0, 2, 8:16, :] + further + over


def shape(*dims):
    return jax.ShapeDtypeStruct(dims, f32)


def swap(x, axis, first):
    count = lax.axis_size(axis)
    pairs = []
    for i in range(first, count - 1, 2):
        pairs += [(i, i + 1), (i + 1, i)]
    return lax.ppermute(x, axis, pairs)


def call(kernel, outs, scratch, args, flops, moved, specs=None, aliases=None, limit=16):
    return pl.pallas_call(
        kernel,
        out_shape=outs,
        in_specs=specs or [VMEM] * len(args),
        out_specs=[VMEM] * len(outs),
        scratch_shapes=scratch,
        input_output_aliases=aliases or {},
        compiler_params=pltpu.CompilerParams(vmem_limit_bytes=limit << 20),
        cost_estimate=pl.CostEstimate(flops=flops, bytes_accessed=moved, transcendentals=0),
    )(*args)


def on_device(volume):
    w = jnp.asarray(column_weights(), bf16)
    we = jnp.asarray(edge_weights(), bf16)
    buf = pltpu.VMEM
    levels = [buf((10, 80, 128), f32), buf((7, 48, 128), f32), buf((5, 32, 128), f32)]
    shells, volume = call(
        shell_kernel,
        [shape(24, 128), shape(16, 64, 1024)],
        [buf((16, 64, 128), f32)]
        + [buf((768, 256), bf16), buf((1024, 768), bf16), buf((1024, 256), f32)]
        + levels
        + [buf((896, 128), f32), pltpu.SemaphoreType.DMA((3,))],
        (volume,),
        10**8,
        1 << 20,
        specs=[pl.BlockSpec(memory_space=pltpu.HBM)],
        limit=48,
    )
    xa = swap(shells, "gx", 0)
    block = [buf((2, 10, 80, 128), f32), buf((2, 10, 48, 128), f32), buf((480, 768), bf16), buf((480, 256), f32)]
    e, f2s, f3s = shape(2, 10, 48, 128), shape(2, 7, 32, 128), shape(1, 5, 32, 128)
    ea, side, again = call(
        first_kernel,
        [e, shape(10, 48, 128), shape(24, 128)],
        block,
        (volume, w, shells),
        4 * 10**9,
        1 << 21,
    )
    xb = swap(again, "gx", 1)
    ea, _, eb, f2, f3 = call(
        second_kernel,
        [e, shape(10, 48, 128), e, f2s, f3s],
        block
        + [buf((10, 48, 128), f32)]
        + [buf((5, 7, 48, 128), f32), buf((5, 7, 32, 128), f32), buf((448, 768), bf16), buf((224, 384), bf16)]
        + [buf((448, 256), f32), buf((224, 256), f32), buf((7, 32, 128), f32)]
        + [buf((3, 5, 32, 128), f32), buf((3, 5, 32, 128), f32), buf((160, 768), bf16), buf((160, 384), bf16)]
        + [buf((160, 256), f32), buf((160, 256), f32)],
        (volume, w, we, ea, side),
        5 * 10**9,
        1 << 21,
        aliases={3: 0, 4: 1},
    )
    keepers = {2: 0, 3: 1, 4: 2, 5: 3}
    ea, eb, f2, f3, ya, yb = call(
        columns_kernel,
        [e, e, f2s, f3s, shape(80, 128), shape(80, 128)],
        [buf((896, 128), f32)],
        (xa, xb, ea, eb, f2, f3),
        10**8,
        1 << 20,
        aliases=keepers,
    )
    ya, yb = swap(ya, "gy", 0), swap(yb, "gy", 1)
    ea, eb, f2, f3, za, zb = call(
        rows_kernel,
        [e, e, f2s, f3s, shape(208, 128), shape(208, 128)],
        [],
        (ya, yb, ea, eb, f2, f3),
        10**8,
        1 << 20,
        aliases=keepers,
    )
    zb = swap(zb, "gz", 1)
    za = swap(za, "gz", 0)
    return tuple(
        call(
            sections_kernel,
            [shape(8, 32, 512), shape(4, 16, 256), shape(2, 8, 128)],
            [],
            (za, zb, ea, eb, f2, f3),
            10**8,
            1 << 20,
        )
    )


def solution(mesh):
    spec = P("gz", "gy", "gx")
    return jax.shard_map(
        on_device, mesh=mesh, in_specs=(spec,), out_specs=(spec,) * 3, check_vma=False
    )
```

```python
import numpy as np
import jax
import jax.numpy as jnp
from jax import lax
from jax.experimental import pallas as pl
from jax.experimental.pallas import tpu as pltpu
from jax.sharding import PartitionSpec as P


taps = (0.0625, 0.25, 0.375, 0.25, 0.0625)
f32, bf16 = jnp.float32, jnp.bfloat16
VMEM = pl.BlockSpec(memory_space=pltpu.VMEM)


def tap(k):
    outer, inner = (k == 0) | (k == 4), (k == 1) | (k == 3)
    return jnp.where(outer, taps[0], jnp.where(inner, taps[1], jnp.where(k == 2, taps[2], 0.0)))


def reduce_weights(w, wrap):
    lane_at = lax.broadcasted_iota(jnp.int32, (128, 128), 1)
    row = lax.broadcasted_iota(jnp.int32, (128, 128), 0)

    def beside(c, n):
        under = jnp.where(lane_at == 0, tap(c - n + 2), 0.0)
        return jnp.where(lane_at == 127, jnp.where(c == 0, taps[4], 0.0), under)

    for h in range(2):
        c = row + h * 128
        main, out = tap(c - 2 * lane_at + 2).astype(bf16), beside(c, 256).astype(bf16)
        for q in range(3):
            at = q * 256 + h * 128
            w[at : at + 128, 0:128] = main
            w[at : at + 128, 128:256] = out
    high = (row >= 64) & (lane_at >= 64)
    low = (row < 64) & (lane_at < 64)
    k = jnp.where(high, row - 2 * lane_at + 130, jnp.where(low, row - 2 * lane_at + 2, -1))
    main, out = tap(k).astype(bf16), beside(row, 128).astype(bf16)
    for q in range(3):
        wrap[q * 128 : q * 128 + 128, 0:128] = main
        wrap[q * 128 : q * 128 + 128, 128:256] = out


def composite(levels):
    h = np.ones(1)
    for level in range(levels):
        up = np.zeros(4 * 2**level + 1)
        up[:: 2**level] = taps
        h = np.convolve(h, up)
    return h


def shell_weights(first, tall):
    lanes = [(1, 0), (1, -1), (2, 0), (2, 1), (2, -1), (3, 0), (3, 1), (3, -1)]
    c = first + lax.broadcasted_iota(jnp.int32, (tall, 128), 0)
    at = lax.broadcasted_iota(jnp.int32, (tall, 128), 1)
    w = jnp.zeros((tall, 128), f32)
    for r, (level, place) in enumerate(lanes):
        h = composite(level)
        start = place * 2**level - len(h) // 2 + (256 if place >= 0 else 0)
        for t in range(len(h)):
            if first <= start + t < first + tall and (start + t < 256 if place >= 0 else start + t >= 0):
                w = jnp.where((at == r) & (c == start + t), float(h[t]), w)
    high = w.astype(bf16)
    return high, (w - high.astype(f32)).astype(bf16)


def split(x):
    a = x.astype(bf16)
    r = x - a.astype(f32)
    b = r.astype(bf16)
    return a, b, (r - b.astype(f32)).astype(bf16)


def weigh(p):
    total = None
    for a, b, t in ((p[0], p[4], taps[0]), (p[1], p[3], taps[1]), (p[2], None, taps[2])):
        if a is None and b is None:
            continue
        s = a if b is None else b if a is None else a + b
        total = t * s if total is None else total + t * s
    return total


def keep(axis, count):
    at = lax.axis_index(axis)
    return (
        jnp.where(at > 0, 1.0, 0.0).astype(f32),
        jnp.where(at < count - 1, 1.0, 0.0).astype(f32),
    )


def sections(load, store, first, last, half, above, ends):
    got = {i: load(i) for i in range(first, last + 1)}
    for i in range(-1, half + above):
        v = weigh([got.get(2 * i - 2 + k) for k in range(5)])
        if i < 0:
            v = v * ends[0]
        if i >= half:
            v = v * ends[1]
        store(i, v)


def rows(src, dst, at, half, ends):
    n = 2 * half
    dst[at, 8 : 8 + half, :] = weigh(
        [src[at, pl.ds(6 + k, half, stride=2), :] for k in range(5)]
    )
    low = taps[3] * src[at, 7:8, :] + taps[4] * src[at, 8:9, :]
    dst[at, 0:8, :] = jnp.where(
        lax.broadcasted_iota(jnp.int32, (8, 128), 0) == 7, low * ends[0], 0.0
    )
    up = [src[at, 6 + n + k : 7 + n + k, :] for k in range(4)]
    high = weigh(up + [None]) * ends[1]
    higher = (taps[0] * up[2] + taps[1] * up[3]) * ends[1]
    row = lax.broadcasted_iota(jnp.int32, (8, 128), 0)
    dst[at, 8 + half : 16 + half, :] = jnp.where(row == 0, high, jnp.where(row == 1, higher, 0.0))


def pack(parts, dst, at):
    wide = len(parts) * 128
    tall = parts[0].shape[0]
    for j, x in enumerate(parts):
        for q, piece in enumerate(split(x)):
            dst[at : at + tall, q * wide + j * 128 : q * wide + (j + 1) * 128] = piece


def low_lanes(tall):
    return lax.broadcasted_iota(jnp.int32, (tall, 128), 1) < 64


def matmul(x, w):
    return jnp.dot(x, w, preferred_element_type=f32)


def pyramid(src, zs, flat, zend, yend):
    z1, z2, z3 = zs
    y1, y2, y3 = (flat.at[pl.ds(o, n * t)].reshape(n, t, 128) for o, n, t in TALL)
    for s in range(10):
        z1[s, 0:8, :] = jnp.zeros((8, 128), f32)
        z1[s, 72:80, :] = jnp.zeros((8, 128), f32)
    for r in range(0, 64, 8):

        def store(i, v, r=r):
            z1[i + 1, 8 + r : 16 + r, :] = v

        sections(lambda i, r=r: src[i, r : r + 8, :], store, 0, 15, 8, 1, zend)
    for s in range(10):
        rows(z1, y1, s, 32, yend)
    for a, zb, b, used, first, half_z, half_y in (
        (y1, z2, y2, 48, 8, 4, 16),
        (y2, z3, y3, 32, 5, 2, 8),
    ):
        for r in range(0, used, 8):

            def store(i, v, r=r, zb=zb):
                zb[i + 1, r : r + 8, :] = v

            sections(lambda i, r=r, a=a: a[i + 1, r : r + 8, :], store, -1, first, half_z, 2, zend)
        for s in range(half_z + 3):
            rows(zb, b, s, half_y, yend)


TALL = ((0, 10, 48), (480, 7, 32), (704, 5, 32))
MIXED = ((3, 96), (5, 64))


def shell_kernel(volume, out, reduce_w, wrap_w, left, right, own, w, lines, prod, z1, z2, z3, flat, sems):
    copies = []
    for j, (first, dst) in enumerate(((0, left), (896, right))):
        copies.append(pltpu.make_async_copy(volume.at[:, :, pl.ds(first, 128)], dst, sems.at[j]))
    for c in copies:
        c.start()
    zend, yend = keep("gz", lax.axis_size("gz")), keep("gy", lax.axis_size("gy"))
    reduce_weights(reduce_w, wrap_w)
    w[...] = jnp.zeros((384, 256), bf16)
    for first, to in ((0, 0), (240, 112)):
        for j, part in enumerate(shell_weights(first, 16)):
            for q in range(3):
                w[q * 128 + to : q * 128 + to + 16, j * 128 : j * 128 + 128] = part
    for s in range(5):
        flat[704 + s * 32 + 24 : 704 + s * 32 + 32, :] = jnp.zeros((8, 128), f32)
    flat[864:896, :] = jnp.zeros((32, 128), f32)
    out[16:24, :] = jnp.zeros((8, 128), f32)
    copies[0].wait()
    copies[1].wait()
    low = low_lanes(64)
    for s in range(16):
        pack([jnp.where(low, left[s], right[s])], lines, s * 64)
    prod[...] = matmul(lines[...], w[...])
    for s in range(16):
        lines_s = prod[s * 64 : s * 64 + 64, :]
        own[s] = lines_s[:, :128] + lines_s[:, 128:]
    pyramid(own, (z1, z2, z3), flat, zend, yend)
    at = lax.broadcasted_iota(jnp.int32, (1, 128), 1)
    mixed = dict(MIXED)
    for j in range(7):
        t = flat[j * 128 : j * 128 + 128, :].T
        pick = [(t[0:1], None, t[1:2]), (t[2:3], t[3:4], t[4:5]), (t[5:6], t[6:7], t[7:8])]
        level = 0 if j < 4 else 1 if j < 6 else 2
        for q in range(3):
            row = pick[level][q]
            row = jnp.zeros((1, 128), f32) if row is None else row
            if j in mixed:
                row = jnp.where(at < mixed[j], row, pick[level + 1][q])
            out[3 * j + q : 3 * j + q + 1, :] = row


def level_one_block(volume, at, zs, ys, ops, res, w, zend, yend):
    for h in range(2):
        cols = pl.ds(at * 256 + h * 128, 128)
        for s in range(10):
            zs[h, s, 0:8, :] = jnp.zeros((8, 128), f32)
            zs[h, s, 72:80, :] = jnp.zeros((8, 128), f32)
        for r in range(0, 64, 8):

            def store(i, v, r=r, h=h):
                zs[h, i + 1, 8 + r : 16 + r, :] = v

            sections(lambda i, r=r, cols=cols: volume[i, r : r + 8, cols], store, 0, 15, 8, 1, zend)
    for s in range(10):
        for h in range(2):
            rows(zs.at[h], ys.at[h], s, 32, yend)
        pack([ys[0, s], ys[1, s]], ops, s * 48)
    res[...] = matmul(ops[...], w[...])


def first_half(volume, w, ea, side, zs, ys, ops, res, zend, yend):
    low = low_lanes(48)
    for b in range(2):
        level_one_block(volume, b, zs, ys, ops, res, w, zend, yend)
        for s in range(10):
            main = res[s * 48 : s * 48 + 48, :128]
            beside = res[s * 48 : s * 48 + 48, 128:]
            if b == 0:
                ea[0, s] = main
                side[s] = beside
            else:
                first = side[s]
                ea[1, s] = main + jnp.where(low, first, 0.0)
                ea[0, s] = ea[0, s] + jnp.where(low, 0.0, beside)
                side[s] = jnp.where(low, beside, first)


def early():
    return lax.axis_index("gx") < lax.axis_size("gx") // 2


def first_kernel(volume, w, shells, ea, side, again, zs, ys, ops, res):
    again[...] = shells[...]
    zend, yend = keep("gz", lax.axis_size("gz")), keep("gy", lax.axis_size("gy"))

    @pl.when(early())
    def _():
        first_half(volume, w, ea, side, zs, ys, ops, res, zend, yend)


def next_level(blocks, edge, zs, ys, ops, edge_ops, res, edge_res, w, we, dst, edge_dst,
               sections_in, half_z, half_y, used_in, tall, zend, yend, xend):
    count = len(blocks)
    many = half_z + 3
    for j, src in enumerate(blocks + [edge]):
        for r in range(0, used_in, 8):

            def store(i, v, r=r, j=j):
                zs[j, i + 1, r : r + 8, :] = v

            sections(lambda i, r=r, src=src: src[i + 1, r : r + 8, :], store, -1,
                     sections_in - 2, half_z, 2, zend)
        for s in range(many):
            rows(zs.at[j], ys.at[j], s, half_y, yend)
    size = many * tall
    for p in range(count // 2):
        for s in range(many):
            pack([ys[2 * p, s], ys[2 * p + 1, s]], ops, p * size + s * tall)
    for s in range(many):
        pack([ys[count, s]], edge_ops, s * tall)
    res[...] = matmul(ops[...], w[...])
    edge_res[...] = matmul(edge_ops[...], we[...])
    low = low_lanes(tall)
    last = count // 2 - 1
    for s in range(many):
        mains, besides = [], []
        for p in range(last + 1):
            at = p * size + s * tall
            mains.append(res[at : at + tall, :128])
            besides.append(res[at : at + tall, 128:])
        at = s * tall
        edge_beside = edge_res[at : at + tall, 128:]
        for p in range(last + 1):
            under = besides[p - 1] if p else edge_beside
            over = besides[p + 1] if p < last else edge_beside
            dst[p, s] = mains[p] + jnp.where(low, under, over)
        if edge_dst is not None:
            wrapped = edge_res[at : at + tall, :128] + jnp.where(low, besides[last], besides[0])
            edge_dst[s] = wrapped * jnp.where(low, xend[1], xend[0])


def second_kernel(volume, w, we, ea_in, side_in, ea, side, eb, f2, f3,
                  zs, ys, ops, res, h1, z2, y2, ops2, opse2, res2, rese2, h2,
                  z3, y3, ops3, opse3, res3, rese3):
    zend, yend, xend = (keep(a, lax.axis_size(a)) for a in ("gz", "gy", "gx"))
    low = low_lanes(48)

    @pl.when(jnp.logical_not(early()))
    def _():
        first_half(volume, w, ea, side, zs, ys, ops, res, zend, yend)

    for b in range(2):
        level_one_block(volume, 2 + b, zs, ys, ops, res, w, zend, yend)
        for s in range(10):
            main = res[s * 48 : s * 48 + 48, :128]
            beside = res[s * 48 : s * 48 + 48, 128:]
            if b == 0:
                eb[0, s] = main + jnp.where(low, side[s], 0.0)
                ea[1, s] = ea[1, s] + jnp.where(low, 0.0, beside)
                h1[s] = beside
            else:
                eb[1, s] = main + jnp.where(low, h1[s], 0.0)
                eb[0, s] = eb[0, s] + jnp.where(low, 0.0, beside)
                h1[s] = jnp.where(low, beside * xend[1], side[s] * xend[0])
    next_level([ea.at[0], ea.at[1], eb.at[0], eb.at[1]], h1, z2, y2, ops2, opse2, res2, rese2,
               w, we, f2, h2, 10, 4, 16, 48, 32, zend, yend, xend)
    next_level([f2.at[0], f2.at[1]], h2, z3, y3, ops3, opse3, res3, rese3,
               w, we, f3, None, 7, 2, 8, 32, 32, zend, yend, xend)


def columns_kernel(pa, pb, ea_in, eb_in, f2_in, f3_in, ea, eb, f2, f3, ya, yb, flat):
    odd = lax.rem(lax.axis_index("gx"), 2) == 1
    for j in range(7):
        a, b = pa[3 * j : 3 * j + 3, :], pb[3 * j : 3 * j + 3, :]
        under, over = jnp.where(odd, a, b), jnp.where(odd, b, a)
        full = jnp.concatenate([under[:2], jnp.zeros((125, 128), f32), over[2:]], axis=0)
        flat[j * 128 : j * 128 + 128, :] = full.T
    low = low_lanes(48)
    for s in range(10):
        v = flat[s * 48 : s * 48 + 48, :]
        ea[0, s] = ea[0, s] + jnp.where(low, v, 0.0)
        eb[1, s] = eb[1, s] + jnp.where(low, 0.0, v)
    low = low_lanes(32)
    for s in range(7):
        v = flat[480 + s * 32 : 512 + s * 32, :]
        f2[0, s] = f2[0, s] + jnp.where(low, v, 0.0)
        f2[1, s] = f2[1, s] + jnp.where(low, 0.0, v)
    for s in range(5):
        f3[0, s] = f3[0, s] + flat[704 + s * 32 : 736 + s * 32, :]

    def emit(dst, high):
        for blk in range(4):
            e = ea if blk < 2 else eb
            for s in range(10):
                at = 40 if high else 7
                dst[blk * 10 + s : blk * 10 + s + 1, :] = e[blk % 2, s, at : at + 1, :]
        for j in range(2 if high else 1):
            for blk in range(2):
                for s in range(7):
                    at, to = 24 + j if high else 7, 40 + j * 14 + blk * 7 + s
                    dst[to : to + 1, :] = f2[blk, s, at : at + 1, :]
            for s in range(5):
                at, to = 16 + j if high else 7, 68 + j * 5 + s
                dst[to : to + 1, :] = f3[0, s, at : at + 1, :]

    odd_row = lax.rem(lax.axis_index("gy"), 2) == 1
    for dst, when in ((ya, odd_row), (yb, jnp.logical_not(odd_row))):
        pl.when(when)(lambda dst=dst: emit(dst, False))
        pl.when(jnp.logical_not(when))(lambda dst=dst: emit(dst, True))


def rows_kernel(pa, pb, ea_in, eb_in, f2_in, f3_in, ea, eb, f2, f3, za, zb):
    odd = lax.rem(lax.axis_index("gy"), 2) == 1

    def got(at):
        a, b = pa[at : at + 1, :], pb[at : at + 1, :]
        return jnp.where(odd, a, b), jnp.where(odd, b, a)

    def add(ref, blk, s, at, v):
        ref[blk, s, at : at + 1, :] = ref[blk, s, at : at + 1, :] + v

    for blk in range(4):
        e = ea if blk < 2 else eb
        for s in range(10):
            under, over = got(blk * 10 + s)
            add(e, blk % 2, s, 8, under)
            add(e, blk % 2, s, 39, over)
    for j in range(2):
        for blk in range(2):
            for s in range(7):
                under, over = got(40 + j * 14 + blk * 7 + s)
                add(f2, blk, s, 8 + j, under)
                if j == 0:
                    add(f2, blk, s, 23, over)
        for s in range(5):
            under, over = got(68 + j * 5 + s)
            add(f3, 0, s, 8 + j, under)
            if j == 0:
                add(f3, 0, s, 15, over)

    def emit(dst, high):
        for blk in range(4):
            e = ea if blk < 2 else eb
            dst[blk * 32 : blk * 32 + 32, :] = e[blk % 2, 9 if high else 0, 8:40, :]
        for j in range(2 if high else 1):
            for blk in range(2):
                to = 128 + j * 32 + blk * 16
                dst[to : to + 16, :] = f2[blk, 5 + j if high else 0, 8:24, :]
            to = 192 + j * 8
            dst[to : to + 8, :] = f3[0, 3 + j if high else 0, 8:16, :]

    odd_slab = lax.rem(lax.axis_index("gz"), 2) == 1
    for dst, when in ((za, odd_slab), (zb, jnp.logical_not(odd_slab))):
        pl.when(when)(lambda dst=dst: emit(dst, False))
        pl.when(jnp.logical_not(when))(lambda dst=dst: emit(dst, True))


def inner_kernel(ea, eb, one, held, sem):
    for blk in range(4):
        e = ea if blk < 2 else eb
        for z in range(1, 7):
            held[z - 1, :, blk * 128 : blk * 128 + 128] = e[blk % 2, z + 1, 8:40, :]
    copy = pltpu.make_async_copy(held, one.at[pl.ds(1, 6)], sem)
    copy.start()
    copy.wait()


def sections_kernel(pa, pb, ea, eb, f2, f3, one_in, one, two_out, three_out, held, two, three, sems):
    odd = lax.rem(lax.axis_index("gz"), 2) == 1

    def got(at, tall):
        a, b = pa[at : at + tall, :], pb[at : at + tall, :]
        return jnp.where(odd, a, b), jnp.where(odd, b, a)

    for blk in range(4):
        e = ea if blk < 2 else eb
        under, over = got(blk * 32, 32)
        cols = slice(blk * 128, blk * 128 + 128)
        held[0, :, cols] = e[blk % 2, 1, 8:40, :] + under
        held[1, :, cols] = e[blk % 2, 8, 8:40, :] + over
    copies = [pltpu.make_async_copy(held.at[j], one.at[7 * j], sems.at[j]) for j in range(2)]
    for c in copies:
        c.start()
    for blk in range(2):
        under, over = got(128 + blk * 16, 16)
        further, _ = got(160 + blk * 16, 16)
        for z in range(4):
            v = f2[blk, z + 1, 8:24, :]
            v = v + under if z == 0 else v + further if z == 1 else v + over if z == 3 else v
            two[z, :, blk * 128 : blk * 128 + 128] = v
    under, over = got(192, 8)
    further, _ = got(200, 8)
    three[0] = f3[0, 1, 8:16, :] + under
    three[1] = f3[0, 2, 8:16, :] + further + over
    copies += [
        pltpu.make_async_copy(two, two_out, sems.at[2]),
        pltpu.make_async_copy(three, three_out, sems.at[3]),
    ]
    for c in copies[2:]:
        c.start()
    for c in copies:
        c.wait()


def shape(*dims):
    return jax.ShapeDtypeStruct(dims, f32)


def swap(x, axis, first):
    count = lax.axis_size(axis)
    pairs = []
    for i in range(first, count - 1, 2):
        pairs += [(i, i + 1), (i + 1, i)]
    return lax.ppermute(x, axis, pairs)


def call(kernel, outs, scratch, args, flops, moved, specs=None, aliases=None, limit=16, outs_in=None):
    return pl.pallas_call(
        kernel,
        out_shape=outs,
        in_specs=specs or [VMEM] * len(args),
        out_specs=outs_in or [VMEM] * len(outs),
        scratch_shapes=scratch,
        input_output_aliases=aliases or {},
        compiler_params=pltpu.CompilerParams(vmem_limit_bytes=limit << 20),
        cost_estimate=pl.CostEstimate(flops=flops, bytes_accessed=moved, transcendentals=0),
    )(*args)


def on_device(volume):
    buf = pltpu.VMEM
    levels = [buf((10, 80, 128), f32), buf((7, 48, 128), f32), buf((5, 32, 128), f32)]
    shells, w, we = call(
        shell_kernel,
        [shape(24, 128), jax.ShapeDtypeStruct((768, 256), bf16), jax.ShapeDtypeStruct((384, 256), bf16)],
        [buf((16, 64, 128), f32)] * 3
        + [buf((384, 256), bf16), buf((1024, 384), bf16), buf((1024, 256), f32)]
        + levels
        + [buf((896, 128), f32), pltpu.SemaphoreType.DMA((2,))],
        (volume,),
        10**8,
        1 << 20,
        specs=[pl.BlockSpec(memory_space=pltpu.HBM)],
        limit=50,
    )
    xa = swap(shells, "gx", 0)
    block = [buf((2, 10, 80, 128), f32), buf((2, 10, 48, 128), f32), buf((480, 768), bf16), buf((480, 256), f32)]
    e, f2s, f3s = shape(2, 10, 48, 128), shape(2, 7, 32, 128), shape(1, 5, 32, 128)
    ea, side, again = call(
        first_kernel,
        [e, shape(10, 48, 128), shape(24, 128)],
        block,
        (volume, w, shells),
        4 * 10**9,
        1 << 21,
    )
    xb = swap(again, "gx", 1)
    ea, _, eb, f2, f3 = call(
        second_kernel,
        [e, shape(10, 48, 128), e, f2s, f3s],
        block
        + [buf((10, 48, 128), f32)]
        + [buf((5, 7, 48, 128), f32), buf((5, 7, 32, 128), f32), buf((448, 768), bf16), buf((224, 384), bf16)]
        + [buf((448, 256), f32), buf((224, 256), f32), buf((7, 32, 128), f32)]
        + [buf((3, 5, 32, 128), f32), buf((3, 5, 32, 128), f32), buf((160, 768), bf16), buf((160, 384), bf16)]
        + [buf((160, 256), f32), buf((160, 256), f32)],
        (volume, w, we, ea, side),
        5 * 10**9,
        1 << 21,
        aliases={3: 0, 4: 1},
    )
    keepers = {2: 0, 3: 1, 4: 2, 5: 3}
    ea, eb, f2, f3, ya, yb = call(
        columns_kernel,
        [e, e, f2s, f3s, shape(80, 128), shape(80, 128)],
        [buf((896, 128), f32)],
        (xa, xb, ea, eb, f2, f3),
        10**8,
        1 << 20,
        aliases=keepers,
    )
    ya, yb = swap(ya, "gy", 0), swap(yb, "gy", 1)
    ea, eb, f2, f3, za, zb = call(
        rows_kernel,
        [e, e, f2s, f3s, shape(208, 128), shape(208, 128)],
        [],
        (ya, yb, ea, eb, f2, f3),
        10**8,
        1 << 20,
        aliases=keepers,
    )
    zb = swap(zb, "gz", 1)
    za = swap(za, "gz", 0)
    hbm = pl.BlockSpec(memory_space=pltpu.HBM)
    whole = shape(8, 32, 512)
    (one,) = call(
        inner_kernel,
        [whole],
        [buf((6, 32, 512), f32), pltpu.SemaphoreType.DMA],
        (ea, eb),
        10**8,
        1 << 20,
        outs_in=[hbm],
    )
    return tuple(
        call(
            sections_kernel,
            [whole, shape(4, 16, 256), shape(2, 8, 128)],
            [buf((2, 32, 512), f32), buf((4, 16, 256), f32), buf((2, 8, 128), f32), pltpu.SemaphoreType.DMA((4,))],
            (za, zb, ea, eb, f2, f3, one),
            10**8,
            1 << 20,
            specs=[VMEM] * 6 + [hbm],
            outs_in=[hbm] * 3,
            aliases={6: 0},
        )
    )


def solution(mesh):
    spec = P("gz", "gy", "gx")
    return jax.shard_map(
        on_device, mesh=mesh, in_specs=(spec,), out_specs=(spec,) * 3, check_vma=False
    )
```

```python
import numpy as np
import jax
import jax.numpy as jnp
from jax import lax
from jax.experimental import pallas as pl
from jax.experimental.pallas import tpu as pltpu
from jax.sharding import PartitionSpec as P


taps = (0.0625, 0.25, 0.375, 0.25, 0.0625)
f32, bf16 = jnp.float32, jnp.bfloat16
VMEM = pl.BlockSpec(memory_space=pltpu.VMEM)


def tap(k):
    outer, inner = (k == 0) | (k == 4), (k == 1) | (k == 3)
    return jnp.where(outer, taps[0], jnp.where(inner, taps[1], jnp.where(k == 2, taps[2], 0.0)))


def reduce_weights(w, wrap):
    lane_at = lax.broadcasted_iota(jnp.int32, (128, 128), 1)
    row = lax.broadcasted_iota(jnp.int32, (128, 128), 0)

    def beside(c, n):
        under = jnp.where(lane_at == 0, tap(c - n + 2), 0.0)
        return jnp.where(lane_at == 127, jnp.where(c == 0, taps[4], 0.0), under)

    for h in range(2):
        c = row + h * 128
        main, out = tap(c - 2 * lane_at + 2).astype(bf16), beside(c, 256).astype(bf16)
        for q in range(3):
            at = q * 256 + h * 128
            w[at : at + 128, 0:128] = main
            w[at : at + 128, 128:256] = out
    high = (row >= 64) & (lane_at >= 64)
    low = (row < 64) & (lane_at < 64)
    k = jnp.where(high, row - 2 * lane_at + 130, jnp.where(low, row - 2 * lane_at + 2, -1))
    main, out = tap(k).astype(bf16), beside(row, 128).astype(bf16)
    for q in range(3):
        wrap[q * 128 : q * 128 + 128, 0:128] = main
        wrap[q * 128 : q * 128 + 128, 128:256] = out


def composite(levels):
    h = np.ones(1)
    for level in range(levels):
        up = np.zeros(4 * 2**level + 1)
        up[:: 2**level] = taps
        h = np.convolve(h, up)
    return h


def shell_weights(first, tall):
    lanes = [(1, 0), (1, -1), (2, 0), (2, 1), (2, -1), (3, 0), (3, 1), (3, -1)]
    c = first + lax.broadcasted_iota(jnp.int32, (tall, 128), 0)
    at = lax.broadcasted_iota(jnp.int32, (tall, 128), 1)
    w = jnp.zeros((tall, 128), f32)
    for r, (level, place) in enumerate(lanes):
        h = composite(level)
        start = place * 2**level - len(h) // 2 + (256 if place >= 0 else 0)
        for t in range(len(h)):
            if first <= start + t < first + tall and (start + t < 256 if place >= 0 else start + t >= 0):
                w = jnp.where((at == r) & (c == start + t), float(h[t]), w)
    high = w.astype(bf16)
    return high, (w - high.astype(f32)).astype(bf16)


def split(x):
    a = x.astype(bf16)
    r = x - a.astype(f32)
    b = r.astype(bf16)
    return a, b, (r - b.astype(f32)).astype(bf16)


def weigh(p):
    total = None
    for a, b, t in ((p[0], p[4], taps[0]), (p[1], p[3], taps[1]), (p[2], None, taps[2])):
        if a is None and b is None:
            continue
        s = a if b is None else b if a is None else a + b
        total = t * s if total is None else total + t * s
    return total


def keep(axis, count):
    at = lax.axis_index(axis)
    return (
        jnp.where(at > 0, 1.0, 0.0).astype(f32),
        jnp.where(at < count - 1, 1.0, 0.0).astype(f32),
    )


def sections(load, store, first, last, half, above, ends):
    got = {i: load(i) for i in range(first, last + 1)}
    for i in range(-1, half + above):
        v = weigh([got.get(2 * i - 2 + k) for k in range(5)])
        if i < 0:
            v = v * ends[0]
        if i >= half:
            v = v * ends[1]
        store(i, v)


def rows(src, dst, at, half, above, ends):
    n = 2 * half
    dst[at, 8 : 8 + half, :] = weigh(
        [src[at, pl.ds(6 + k, half, stride=2), :] for k in range(5)]
    )
    low = taps[4] * src[at, 8:9, :]
    if above > 1:
        low = low + taps[3] * src[at, 7:8, :]
    dst[at, 0:8, :] = jnp.where(
        lax.broadcasted_iota(jnp.int32, (8, 128), 0) == 7, low * ends[0], 0.0
    )
    up = [src[at, 6 + n + k : 7 + n + k, :] for k in range(2 * above)]
    high = weigh((up + [None] * 4)[:5]) * ends[1]
    row = lax.broadcasted_iota(jnp.int32, (8, 128), 0)
    tile = jnp.where(row == 0, high, 0.0)
    if above > 1:
        tile = jnp.where(row == 1, (taps[0] * up[2] + taps[1] * up[3]) * ends[1], tile)
    dst[at, 8 + half : 16 + half, :] = tile


def pack(parts, dst, at):
    wide = len(parts) * 128
    tall = parts[0].shape[0]
    for j, x in enumerate(parts):
        for q, piece in enumerate(split(x)):
            dst[at : at + tall, q * wide + j * 128 : q * wide + (j + 1) * 128] = piece


def low_lanes(tall):
    return lax.broadcasted_iota(jnp.int32, (tall, 128), 1) < 64


def matmul(x, w):
    return jnp.dot(x, w, preferred_element_type=f32)


def pyramid(src, zs, flat, zend, yend):
    z1, z2, z3 = zs
    y1, y2, y3 = (flat.at[pl.ds(o, n * t)].reshape(n, t, 128) for o, n, t in TALL)
    for s in range(10):
        z1[s, 0:8, :] = jnp.zeros((8, 128), f32)
        z1[s, 72:80, :] = jnp.zeros((8, 128), f32)
    for r in range(0, 64, 8):

        def store(i, v, r=r):
            z1[i + 1, 8 + r : 16 + r, :] = v

        sections(lambda i, r=r: src[i, r : r + 8, :], store, 0, 15, 8, 1, zend)
    for s in range(10):
        rows(z1, y1, s, 32, 1, yend)
    for a, zb, b, used, first, half_z, half_y in (
        (y1, z2, y2, 48, 8, 4, 16),
        (y2, z3, y3, 32, 5, 2, 8),
    ):
        for r in range(0, used, 8):

            def store(i, v, r=r, zb=zb):
                zb[i + 1, r : r + 8, :] = v

            sections(lambda i, r=r, a=a: a[i + 1, r : r + 8, :], store, -1, first, half_z, 2, zend)
        for s in range(half_z + 3):
            rows(zb, b, s, half_y, 2, yend)


TALL = ((0, 10, 48), (480, 7, 32), (704, 5, 32))
MIXED = ((3, 96), (5, 64))


def shell_kernel(volume, out, reduce_w, wrap_w, left, right, own, w, lines, prod, z1, z2, z3, flat, sems):
    copies = []
    for j, (first, dst) in enumerate(((0, left), (896, right))):
        copies.append(pltpu.make_async_copy(volume.at[:, :, pl.ds(first, 128)], dst, sems.at[j]))
    for c in copies:
        c.start()
    zend, yend = keep("gz", lax.axis_size("gz")), keep("gy", lax.axis_size("gy"))
    reduce_weights(reduce_w, wrap_w)
    w[...] = jnp.zeros((384, 256), bf16)
    for first, to in ((0, 0), (240, 112)):
        for j, part in enumerate(shell_weights(first, 16)):
            for q in range(3):
                w[q * 128 + to : q * 128 + to + 16, j * 128 : j * 128 + 128] = part
    for s in range(5):
        flat[704 + s * 32 + 24 : 704 + s * 32 + 32, :] = jnp.zeros((8, 128), f32)
    flat[864:896, :] = jnp.zeros((32, 128), f32)
    out[16:24, :] = jnp.zeros((8, 128), f32)
    copies[0].wait()
    copies[1].wait()
    low = low_lanes(64)
    for s in range(16):
        pack([jnp.where(low, left[s], right[s])], lines, s * 64)
    prod[...] = matmul(lines[...], w[...])
    for s in range(16):
        lines_s = prod[s * 64 : s * 64 + 64, :]
        own[s] = lines_s[:, :128] + lines_s[:, 128:]
    pyramid(own, (z1, z2, z3), flat, zend, yend)
    at = lax.broadcasted_iota(jnp.int32, (1, 128), 1)
    mixed = dict(MIXED)
    for j in range(7):
        t = flat[j * 128 : j * 128 + 128, :].T
        pick = [(t[0:1], None, t[1:2]), (t[2:3], t[3:4], t[4:5]), (t[5:6], t[6:7], t[7:8])]
        level = 0 if j < 4 else 1 if j < 6 else 2
        for q in range(3):
            row = pick[level][q]
            row = jnp.zeros((1, 128), f32) if row is None else row
            if j in mixed:
                row = jnp.where(at < mixed[j], row, pick[level + 1][q])
            out[3 * j + q : 3 * j + q + 1, :] = row


def level_one_block(volume, at, zs, ys, ops, res, w, zend, yend):
    for h in range(2):
        cols = pl.ds(at * 256 + h * 128, 128)
        for s in range(10 if at % 2 == 0 else 0):
            zs[h, s, 0:8, :] = jnp.zeros((8, 128), f32)
            zs[h, s, 72:80, :] = jnp.zeros((8, 128), f32)
        for r in range(0, 64, 8):

            def store(i, v, r=r, h=h):
                zs[h, i + 1, 8 + r : 16 + r, :] = v

            sections(lambda i, r=r, cols=cols: volume[i, r : r + 8, cols], store, 0, 15, 8, 1, zend)
    for s in range(10):
        for h in range(2):
            rows(zs.at[h], ys.at[h], s, 32, 1, yend)
        pack([ys[0, s], ys[1, s]], ops, s * 48)
    res[...] = matmul(ops[...], w[...])


def first_half(volume, w, ea, side, zs, ys, ops, res, zend, yend):
    low = low_lanes(48)
    for b in range(2):
        level_one_block(volume, b, zs, ys, ops, res, w, zend, yend)
        for s in range(10):
            main = res[s * 48 : s * 48 + 48, :128]
            beside = res[s * 48 : s * 48 + 48, 128:]
            if b == 0:
                ea[0, s] = main
                side[s] = beside
            else:
                first = side[s]
                ea[1, s] = main + jnp.where(low, first, 0.0)
                ea[0, s] = ea[0, s] + jnp.where(low, 0.0, beside)
                side[s] = jnp.where(low, beside, first)


def early():
    return lax.axis_index("gx") < lax.axis_size("gx") // 2


def first_kernel(volume, w, shells, ea, side, again, zs, ys, ops, res):
    again[...] = shells[...]
    zend, yend = keep("gz", lax.axis_size("gz")), keep("gy", lax.axis_size("gy"))

    @pl.when(early())
    def _():
        first_half(volume, w, ea, side, zs, ys, ops, res, zend, yend)


def next_level(blocks, edge, zs, ys, ops, edge_ops, res, edge_res, w, we, dst, edge_dst,
               sections_in, half_z, half_y, used_in, tall, zend, yend, xend):
    count = len(blocks)
    many = half_z + 3
    for j, src in enumerate(blocks + [edge]):
        for r in range(0, used_in, 8):

            def store(i, v, r=r, j=j):
                zs[j, i + 1, r : r + 8, :] = v

            sections(lambda i, r=r, src=src: src[i + 1, r : r + 8, :], store, -1,
                     sections_in - 2, half_z, 2, zend)
        for s in range(many):
            rows(zs.at[j], ys.at[j], s, half_y, 2, yend)
    size = many * tall
    for p in range(count // 2):
        for s in range(many):
            pack([ys[2 * p, s], ys[2 * p + 1, s]], ops, p * size + s * tall)
    for s in range(many):
        pack([ys[count, s]], edge_ops, s * tall)
    res[...] = matmul(ops[...], w[...])
    edge_res[...] = matmul(edge_ops[...], we[...])
    low = low_lanes(tall)
    last = count // 2 - 1
    for s in range(many):
        mains, besides = [], []
        for p in range(last + 1):
            at = p * size + s * tall
            mains.append(res[at : at + tall, :128])
            besides.append(res[at : at + tall, 128:])
        at = s * tall
        edge_beside = edge_res[at : at + tall, 128:]
        for p in range(last + 1):
            under = besides[p - 1] if p else edge_beside
            over = besides[p + 1] if p < last else edge_beside
            dst[p, s] = mains[p] + jnp.where(low, under, over)
        if edge_dst is not None:
            wrapped = edge_res[at : at + tall, :128] + jnp.where(low, besides[last], besides[0])
            edge_dst[s] = wrapped * jnp.where(low, xend[1], xend[0])


def second_kernel(volume, w, we, ea_in, side_in, ea, side, eb, f2, f3,
                  zs, ys, ops, res, h1, z2, y2, ops2, opse2, res2, rese2, h2,
                  z3, y3, ops3, opse3, res3, rese3):
    zend, yend, xend = (keep(a, lax.axis_size(a)) for a in ("gz", "gy", "gx"))
    low = low_lanes(48)

    @pl.when(jnp.logical_not(early()))
    def _():
        first_half(volume, w, ea, side, zs, ys, ops, res, zend, yend)

    for b in range(2):
        level_one_block(volume, 2 + b, zs, ys, ops, res, w, zend, yend)
        for s in range(10):
            main = res[s * 48 : s * 48 + 48, :128]
            beside = res[s * 48 : s * 48 + 48, 128:]
            if b == 0:
                eb[0, s] = main + jnp.where(low, side[s], 0.0)
                ea[1, s] = ea[1, s] + jnp.where(low, 0.0, beside)
                h1[s] = beside
            else:
                eb[1, s] = main + jnp.where(low, h1[s], 0.0)
                eb[0, s] = eb[0, s] + jnp.where(low, 0.0, beside)
                h1[s] = jnp.where(low, beside * xend[1], side[s] * xend[0])
    next_level([ea.at[0], ea.at[1], eb.at[0], eb.at[1]], h1, z2, y2, ops2, opse2, res2, rese2,
               w, we, f2, h2, 10, 4, 16, 48, 32, zend, yend, xend)
    next_level([f2.at[0], f2.at[1]], h2, z3, y3, ops3, opse3, res3, rese3,
               w, we, f3, None, 7, 2, 8, 32, 32, zend, yend, xend)


def columns_kernel(pa, pb, ea_in, eb_in, f2_in, f3_in, ea, eb, f2, f3, ya, yb, flat):
    odd = lax.rem(lax.axis_index("gx"), 2) == 1
    for j in range(7):
        a, b = pa[3 * j : 3 * j + 3, :], pb[3 * j : 3 * j + 3, :]
        under, over = jnp.where(odd, a, b), jnp.where(odd, b, a)
        full = jnp.concatenate([under[:2], jnp.zeros((125, 128), f32), over[2:]], axis=0)
        flat[j * 128 : j * 128 + 128, :] = full.T
    low = low_lanes(48)
    for s in range(10):
        v = flat[s * 48 : s * 48 + 48, :]
        ea[0, s] = ea[0, s] + jnp.where(low, v, 0.0)
        eb[1, s] = eb[1, s] + jnp.where(low, 0.0, v)
    low = low_lanes(32)
    for s in range(7):
        v = flat[480 + s * 32 : 512 + s * 32, :]
        f2[0, s] = f2[0, s] + jnp.where(low, v, 0.0)
        f2[1, s] = f2[1, s] + jnp.where(low, 0.0, v)
    for s in range(5):
        f3[0, s] = f3[0, s] + flat[704 + s * 32 : 736 + s * 32, :]

    def emit(dst, high):
        for blk in range(4):
            e = ea if blk < 2 else eb
            for s in range(10):
                at = 40 if high else 7
                dst[blk * 10 + s : blk * 10 + s + 1, :] = e[blk % 2, s, at : at + 1, :]
        for j in range(2 if high else 1):
            for blk in range(2):
                for s in range(7):
                    at, to = 24 + j if high else 7, 40 + j * 14 + blk * 7 + s
                    dst[to : to + 1, :] = f2[blk, s, at : at + 1, :]
            for s in range(5):
                at, to = 16 + j if high else 7, 68 + j * 5 + s
                dst[to : to + 1, :] = f3[0, s, at : at + 1, :]

    odd_row = lax.rem(lax.axis_index("gy"), 2) == 1
    for dst, when in ((ya, odd_row), (yb, jnp.logical_not(odd_row))):
        pl.when(when)(lambda dst=dst: emit(dst, False))
        pl.when(jnp.logical_not(when))(lambda dst=dst: emit(dst, True))


def rows_kernel(pa, pb, ea_in, eb_in, f2_in, f3_in, ea, eb, f2, f3, za, zb):
    odd = lax.rem(lax.axis_index("gy"), 2) == 1

    def got(at):
        a, b = pa[at : at + 1, :], pb[at : at + 1, :]
        return jnp.where(odd, a, b), jnp.where(odd, b, a)

    def add(ref, blk, s, at, v):
        ref[blk, s, at : at + 1, :] = ref[blk, s, at : at + 1, :] + v

    for blk in range(4):
        e = ea if blk < 2 else eb
        for s in range(10):
            under, over = got(blk * 10 + s)
            add(e, blk % 2, s, 8, under)
            add(e, blk % 2, s, 39, over)
    for j in range(2):
        for blk in range(2):
            for s in range(7):
                under, over = got(40 + j * 14 + blk * 7 + s)
                add(f2, blk, s, 8 + j, under)
                if j == 0:
                    add(f2, blk, s, 23, over)
        for s in range(5):
            under, over = got(68 + j * 5 + s)
            add(f3, 0, s, 8 + j, under)
            if j == 0:
                add(f3, 0, s, 15, over)

    def emit(dst, high):
        for blk in range(4):
            e = ea if blk < 2 else eb
            dst[blk * 32 : blk * 32 + 32, :] = e[blk % 2, 9 if high else 0, 8:40, :]
        for j in range(2 if high else 1):
            for blk in range(2):
                to = 128 + j * 32 + blk * 16
                dst[to : to + 16, :] = f2[blk, 5 + j if high else 0, 8:24, :]
            to = 192 + j * 8
            dst[to : to + 8, :] = f3[0, 3 + j if high else 0, 8:16, :]

    odd_slab = lax.rem(lax.axis_index("gz"), 2) == 1
    for dst, when in ((za, odd_slab), (zb, jnp.logical_not(odd_slab))):
        pl.when(when)(lambda dst=dst: emit(dst, False))
        pl.when(jnp.logical_not(when))(lambda dst=dst: emit(dst, True))


def inner_kernel(ea, eb, one, held, sem):
    for blk in range(4):
        e = ea if blk < 2 else eb
        for z in range(1, 7):
            held[z - 1, :, blk * 128 : blk * 128 + 128] = e[blk % 2, z + 1, 8:40, :]
    copy = pltpu.make_async_copy(held, one.at[pl.ds(1, 6)], sem)
    copy.start()
    copy.wait()


def sections_kernel(pa, pb, ea, eb, f2, f3, one_in, one, two_out, three_out, held, two, three, sems):
    odd = lax.rem(lax.axis_index("gz"), 2) == 1

    def got(at, tall):
        a, b = pa[at : at + tall, :], pb[at : at + tall, :]
        return jnp.where(odd, a, b), jnp.where(odd, b, a)

    for blk in range(4):
        e = ea if blk < 2 else eb
        under, over = got(blk * 32, 32)
        cols = slice(blk * 128, blk * 128 + 128)
        held[0, :, cols] = e[blk % 2, 1, 8:40, :] + under
        held[1, :, cols] = e[blk % 2, 8, 8:40, :] + over
    copies = [pltpu.make_async_copy(held.at[j], one.at[7 * j], sems.at[j]) for j in range(2)]
    for c in copies:
        c.start()
    for blk in range(2):
        under, over = got(128 + blk * 16, 16)
        further, _ = got(160 + blk * 16, 16)
        for z in range(4):
            v = f2[blk, z + 1, 8:24, :]
            v = v + under if z == 0 else v + further if z == 1 else v + over if z == 3 else v
            two[z, :, blk * 128 : blk * 128 + 128] = v
    under, over = got(192, 8)
    further, _ = got(200, 8)
    three[0] = f3[0, 1, 8:16, :] + under
    three[1] = f3[0, 2, 8:16, :] + further + over
    copies += [
        pltpu.make_async_copy(two, two_out, sems.at[2]),
        pltpu.make_async_copy(three, three_out, sems.at[3]),
    ]
    for c in copies[2:]:
        c.start()
    for c in copies:
        c.wait()


def shape(*dims):
    return jax.ShapeDtypeStruct(dims, f32)


def swap(x, axis, first):
    count = lax.axis_size(axis)
    pairs = []
    for i in range(first, count - 1, 2):
        pairs += [(i, i + 1), (i + 1, i)]
    return lax.ppermute(x, axis, pairs)


def call(kernel, outs, scratch, args, flops, moved, specs=None, aliases=None, limit=16, outs_in=None):
    return pl.pallas_call(
        kernel,
        out_shape=outs,
        in_specs=specs or [VMEM] * len(args),
        out_specs=outs_in or [VMEM] * len(outs),
        scratch_shapes=scratch,
        input_output_aliases=aliases or {},
        compiler_params=pltpu.CompilerParams(vmem_limit_bytes=limit << 20),
        cost_estimate=pl.CostEstimate(flops=flops, bytes_accessed=moved, transcendentals=0),
    )(*args)


def on_device(volume):
    buf = pltpu.VMEM
    levels = [buf((10, 80, 128), f32), buf((7, 48, 128), f32), buf((5, 32, 128), f32)]
    shells, w, we = call(
        shell_kernel,
        [shape(24, 128), jax.ShapeDtypeStruct((768, 256), bf16), jax.ShapeDtypeStruct((384, 256), bf16)],
        [buf((16, 64, 128), f32)] * 3
        + [buf((384, 256), bf16), buf((1024, 384), bf16), buf((1024, 256), f32)]
        + levels
        + [buf((896, 128), f32), pltpu.SemaphoreType.DMA((2,))],
        (volume,),
        10**8,
        1 << 20,
        specs=[pl.BlockSpec(memory_space=pltpu.HBM)],
        limit=50,
    )
    xa = swap(shells, "gx", 0)
    block = [buf((2, 10, 80, 128), f32), buf((2, 10, 48, 128), f32), buf((480, 768), bf16), buf((480, 256), f32)]
    e, f2s, f3s = shape(2, 10, 48, 128), shape(2, 7, 32, 128), shape(1, 5, 32, 128)
    ea, side, again = call(
        first_kernel,
        [e, shape(10, 48, 128), shape(24, 128)],
        block,
        (volume, w, shells),
        4 * 10**9,
        1 << 21,
    )
    xb = swap(again, "gx", 1)
    ea, _, eb, f2, f3 = call(
        second_kernel,
        [e, shape(10, 48, 128), e, f2s, f3s],
        block
        + [buf((10, 48, 128), f32)]
        + [buf((5, 7, 48, 128), f32), buf((5, 7, 32, 128), f32), buf((448, 768), bf16), buf((224, 384), bf16)]
        + [buf((448, 256), f32), buf((224, 256), f32), buf((7, 32, 128), f32)]
        + [buf((3, 5, 32, 128), f32), buf((3, 5, 32, 128), f32), buf((160, 768), bf16), buf((160, 384), bf16)]
        + [buf((160, 256), f32), buf((160, 256), f32)],
        (volume, w, we, ea, side),
        5 * 10**9,
        1 << 21,
        aliases={3: 0, 4: 1},
    )
    keepers = {2: 0, 3: 1, 4: 2, 5: 3}
    ea, eb, f2, f3, ya, yb = call(
        columns_kernel,
        [e, e, f2s, f3s, shape(80, 128), shape(80, 128)],
        [buf((896, 128), f32)],
        (xa, xb, ea, eb, f2, f3),
        10**8,
        1 << 20,
        aliases=keepers,
    )
    ya, yb = swap(ya, "gy", 0), swap(yb, "gy", 1)
    ea, eb, f2, f3, za, zb = call(
        rows_kernel,
        [e, e, f2s, f3s, shape(208, 128), shape(208, 128)],
        [],
        (ya, yb, ea, eb, f2, f3),
        10**8,
        1 << 20,
        aliases=keepers,
    )
    zb = swap(zb, "gz", 1)
    za = swap(za, "gz", 0)
    hbm = pl.BlockSpec(memory_space=pltpu.HBM)
    whole = shape(8, 32, 512)
    (one,) = call(
        inner_kernel,
        [whole],
        [buf((6, 32, 512), f32), pltpu.SemaphoreType.DMA],
        (ea, eb),
        10**8,
        1 << 20,
        outs_in=[hbm],
    )
    return tuple(
        call(
            sections_kernel,
            [whole, shape(4, 16, 256), shape(2, 8, 128)],
            [buf((2, 32, 512), f32), buf((4, 16, 256), f32), buf((2, 8, 128), f32), pltpu.SemaphoreType.DMA((4,))],
            (za, zb, ea, eb, f2, f3, one),
            10**8,
            1 << 20,
            specs=[VMEM] * 6 + [hbm],
            outs_in=[hbm] * 3,
            aliases={6: 0},
        )
    )


def solution(mesh):
    spec = P("gz", "gy", "gx")
    return jax.shard_map(
        on_device, mesh=mesh, in_specs=(spec,), out_specs=(spec,) * 3, check_vma=False
    )
```

```python
import numpy as np
import jax
import jax.numpy as jnp
from jax import lax
from jax.experimental import pallas as pl
from jax.experimental.pallas import tpu as pltpu
from jax.sharding import PartitionSpec as P


taps = (0.0625, 0.25, 0.375, 0.25, 0.0625)
f32, bf16 = jnp.float32, jnp.bfloat16
VMEM = pl.BlockSpec(memory_space=pltpu.VMEM)


def tap(k):
    outer, inner = (k == 0) | (k == 4), (k == 1) | (k == 3)
    return jnp.where(outer, taps[0], jnp.where(inner, taps[1], jnp.where(k == 2, taps[2], 0.0)))


def reduce_weights(w, wrap):
    lane_at = lax.broadcasted_iota(jnp.int32, (128, 128), 1)
    row = lax.broadcasted_iota(jnp.int32, (128, 128), 0)

    def beside(c, n):
        under = jnp.where(lane_at == 0, tap(c - n + 2), 0.0)
        return jnp.where(lane_at == 127, jnp.where(c == 0, taps[4], 0.0), under)

    for h in range(2):
        c = row + h * 128
        main, out = tap(c - 2 * lane_at + 2).astype(bf16), beside(c, 256).astype(bf16)
        for q in range(3):
            at = q * 256 + h * 128
            w[at : at + 128, 0:128] = main
            w[at : at + 128, 128:256] = out
    high = (row >= 64) & (lane_at >= 64)
    low = (row < 64) & (lane_at < 64)
    k = jnp.where(high, row - 2 * lane_at + 130, jnp.where(low, row - 2 * lane_at + 2, -1))
    main, out = tap(k).astype(bf16), beside(row, 128).astype(bf16)
    for q in range(3):
        wrap[q * 128 : q * 128 + 128, 0:128] = main
        wrap[q * 128 : q * 128 + 128, 128:256] = out


def composite(levels):
    h = np.ones(1)
    for level in range(levels):
        up = np.zeros(4 * 2**level + 1)
        up[:: 2**level] = taps
        h = np.convolve(h, up)
    return h


def shell_weights(first, tall):
    lanes = [(1, 0), (1, -1), (2, 0), (2, 1), (2, -1), (3, 0), (3, 1), (3, -1)]
    c = first + lax.broadcasted_iota(jnp.int32, (tall, 128), 0)
    at = lax.broadcasted_iota(jnp.int32, (tall, 128), 1)
    w = jnp.zeros((tall, 128), f32)
    for r, (level, place) in enumerate(lanes):
        h = composite(level)
        start = place * 2**level - len(h) // 2 + (256 if place >= 0 else 0)
        for t in range(len(h)):
            if first <= start + t < first + tall and (start + t < 256 if place >= 0 else start + t >= 0):
                w = jnp.where((at == r) & (c == start + t), float(h[t]), w)
    high = w.astype(bf16)
    return high, (w - high.astype(f32)).astype(bf16)


def split(x):
    a = x.astype(bf16)
    r = x - a.astype(f32)
    b = r.astype(bf16)
    return a, b, (r - b.astype(f32)).astype(bf16)


def weigh(p):
    total = None
    for a, b, t in ((p[0], p[4], taps[0]), (p[1], p[3], taps[1]), (p[2], None, taps[2])):
        if a is None and b is None:
            continue
        s = a if b is None else b if a is None else a + b
        total = t * s if total is None else total + t * s
    return total


def keep(axis, count):
    at = lax.axis_index(axis)
    return (
        jnp.where(at > 0, 1.0, 0.0).astype(f32),
        jnp.where(at < count - 1, 1.0, 0.0).astype(f32),
    )


def sections(load, store, first, last, half, above, ends):
    got = {i: load(i) for i in range(first, last + 1)}
    for i in range(-1, half + above):
        v = weigh([got.get(2 * i - 2 + k) for k in range(5)])
        if i < 0:
            v = v * ends[0]
        if i >= half:
            v = v * ends[1]
        store(i, v)


def rows(src, dst, at, half, above, ends):
    n = 2 * half
    dst[at, 8 : 8 + half, :] = weigh(
        [src[at, pl.ds(6 + k, half, stride=2), :] for k in range(5)]
    )
    low = taps[4] * src[at, 8:9, :]
    if above > 1:
        low = low + taps[3] * src[at, 7:8, :]
    dst[at, 0:8, :] = jnp.where(
        lax.broadcasted_iota(jnp.int32, (8, 128), 0) == 7, low * ends[0], 0.0
    )
    up = [src[at, 6 + n + k : 7 + n + k, :] for k in range(2 * above)]
    high = weigh((up + [None] * 4)[:5]) * ends[1]
    row = lax.broadcasted_iota(jnp.int32, (8, 128), 0)
    tile = jnp.where(row == 0, high, 0.0)
    if above > 1:
        tile = jnp.where(row == 1, (taps[0] * up[2] + taps[1] * up[3]) * ends[1], tile)
    dst[at, 8 + half : 16 + half, :] = tile


def pack(parts, dst, at):
    wide = len(parts) * 128
    tall = parts[0].shape[0]
    for j, x in enumerate(parts):
        for q, piece in enumerate(split(x)):
            dst[at : at + tall, q * wide + j * 128 : q * wide + (j + 1) * 128] = piece


def low_lanes(tall):
    return lax.broadcasted_iota(jnp.int32, (tall, 128), 1) < 64


def matmul(x, w):
    return jnp.dot(x, w, preferred_element_type=f32)


def pyramid(src, zs, flat, zend, yend):
    z1, z2, z3 = zs
    y1, y2, y3 = (flat.at[pl.ds(o, n * t)].reshape(n, t, 128) for o, n, t in TALL)
    for s in range(10):
        z1[s, 0:8, :] = jnp.zeros((8, 128), f32)
        z1[s, 72:80, :] = jnp.zeros((8, 128), f32)
    for r in range(0, 64, 8):

        def store(i, v, r=r):
            z1[i + 1, 8 + r : 16 + r, :] = v

        sections(lambda i, r=r: src[i, r : r + 8, :], store, 0, 15, 8, 1, zend)
    for s in range(10):
        rows(z1, y1, s, 32, 1, yend)
    for a, zb, b, used, first, half_z, half_y in (
        (y1, z2, y2, 48, 8, 4, 16),
        (y2, z3, y3, 32, 5, 2, 8),
    ):
        for r in range(0, used, 8):

            def store(i, v, r=r, zb=zb):
                zb[i + 1, r : r + 8, :] = v

            sections(lambda i, r=r, a=a: a[i + 1, r : r + 8, :], store, -1, first, half_z, 2, zend)
        for s in range(half_z + 3):
            rows(zb, b, s, half_y, 2, yend)


TALL = ((0, 10, 48), (480, 7, 32), (704, 5, 32))
MIXED = ((3, 96), (5, 64))


def shell_kernel(volume, out, reduce_w, wrap_w, left, right, own, w, lines, prod, z1, z2, z3, flat, sems):
    copies = []
    for j in range(4):
        first, dst, part = (0, 896)[j % 2], (left, right)[j % 2], pl.ds(j // 2 * 8, 8)
        copies.append(
            pltpu.make_async_copy(volume.at[part, :, pl.ds(first, 128)], dst.at[part], sems.at[j])
        )
    for c in copies:
        c.start()
    zend, yend = keep("gz", lax.axis_size("gz")), keep("gy", lax.axis_size("gy"))
    reduce_weights(reduce_w, wrap_w)
    w[...] = jnp.zeros((384, 256), bf16)
    for first, to in ((0, 0), (240, 112)):
        for j, part in enumerate(shell_weights(first, 16)):
            for q in range(3):
                w[q * 128 + to : q * 128 + to + 16, j * 128 : j * 128 + 128] = part
    for s in range(5):
        flat[704 + s * 32 + 24 : 704 + s * 32 + 32, :] = jnp.zeros((8, 128), f32)
    flat[864:896, :] = jnp.zeros((32, 128), f32)
    out[16:24, :] = jnp.zeros((8, 128), f32)
    low = low_lanes(64)
    for s in range(16):
        if s % 8 == 0:
            copies[s // 4].wait()
            copies[s // 4 + 1].wait()
        pack([jnp.where(low, left[s], right[s])], lines, s * 64)
    prod[...] = matmul(lines[...], w[...])
    for s in range(16):
        lines_s = prod[s * 64 : s * 64 + 64, :]
        own[s] = lines_s[:, :128] + lines_s[:, 128:]
    pyramid(own, (z1, z2, z3), flat, zend, yend)
    at = lax.broadcasted_iota(jnp.int32, (1, 128), 1)
    mixed = dict(MIXED)
    for j in range(7):
        t = flat[j * 128 : j * 128 + 128, :].T
        pick = [(t[0:1], None, t[1:2]), (t[2:3], t[3:4], t[4:5]), (t[5:6], t[6:7], t[7:8])]
        level = 0 if j < 4 else 1 if j < 6 else 2
        for q in range(3):
            row = pick[level][q]
            row = jnp.zeros((1, 128), f32) if row is None else row
            if j in mixed:
                row = jnp.where(at < mixed[j], row, pick[level + 1][q])
            out[3 * j + q : 3 * j + q + 1, :] = row


def level_one_block(volume, at, zs, ys, ops, res, w, zend, yend):
    for h in range(2):
        cols = pl.ds(at * 256 + h * 128, 128)
        for s in range(10 if at % 2 == 0 else 0):
            zs[h, s, 0:8, :] = jnp.zeros((8, 128), f32)
            zs[h, s, 72:80, :] = jnp.zeros((8, 128), f32)
        for r in range(0, 64, 8):

            def store(i, v, r=r, h=h):
                zs[h, i + 1, 8 + r : 16 + r, :] = v

            sections(lambda i, r=r, cols=cols: volume[i, r : r + 8, cols], store, 0, 15, 8, 1, zend)
    for s in range(10):
        for h in range(2):
            rows(zs.at[h], ys.at[h], s, 32, 1, yend)
        pack([ys[0, s], ys[1, s]], ops, s * 48)
    res[...] = matmul(ops[...], w[...])


def first_half(volume, w, ea, side, zs, ys, ops, res, zend, yend):
    low = low_lanes(48)
    for b in range(2):
        level_one_block(volume, b, zs, ys, ops, res, w, zend, yend)
        for s in range(10):
            main = res[s * 48 : s * 48 + 48, :128]
            beside = res[s * 48 : s * 48 + 48, 128:]
            if b == 0:
                ea[0, s] = main
                side[s] = beside
            else:
                first = side[s]
                ea[1, s] = main + jnp.where(low, first, 0.0)
                ea[0, s] = ea[0, s] + jnp.where(low, 0.0, beside)
                side[s] = jnp.where(low, beside, first)


def early():
    return lax.axis_index("gx") < lax.axis_size("gx") // 2


def first_kernel(volume, w, shells, ea, side, again, zs, ys, ops, res):
    again[...] = shells[...]
    zend, yend = keep("gz", lax.axis_size("gz")), keep("gy", lax.axis_size("gy"))

    @pl.when(early())
    def _():
        first_half(volume, w, ea, side, zs, ys, ops, res, zend, yend)


def next_level(blocks, edge, zs, ys, ops, edge_ops, res, edge_res, w, we, dst, edge_dst,
               sections_in, half_z, half_y, used_in, tall, zend, yend, xend):
    count = len(blocks)
    many = half_z + 3
    for j, src in enumerate(blocks + [edge]):
        for r in range(0, used_in, 8):

            def store(i, v, r=r, j=j):
                zs[j, i + 1, r : r + 8, :] = v

            sections(lambda i, r=r, src=src: src[i + 1, r : r + 8, :], store, -1,
                     sections_in - 2, half_z, 2, zend)
        for s in range(many):
            rows(zs.at[j], ys.at[j], s, half_y, 2, yend)
    size = many * tall
    for p in range(count // 2):
        for s in range(many):
            pack([ys[2 * p, s], ys[2 * p + 1, s]], ops, p * size + s * tall)
    for s in range(many):
        pack([ys[count, s]], edge_ops, s * tall)
    res[...] = matmul(ops[...], w[...])
    edge_res[...] = matmul(edge_ops[...], we[...])
    low = low_lanes(tall)
    last = count // 2 - 1
    for s in range(many):
        mains, besides = [], []
        for p in range(last + 1):
            at = p * size + s * tall
            mains.append(res[at : at + tall, :128])
            besides.append(res[at : at + tall, 128:])
        at = s * tall
        edge_beside = edge_res[at : at + tall, 128:]
        for p in range(last + 1):
            under = besides[p - 1] if p else edge_beside
            over = besides[p + 1] if p < last else edge_beside
            dst[p, s] = mains[p] + jnp.where(low, under, over)
        if edge_dst is not None:
            wrapped = edge_res[at : at + tall, :128] + jnp.where(low, besides[last], besides[0])
            edge_dst[s] = wrapped * jnp.where(low, xend[1], xend[0])


def second_kernel(volume, w, we, ea_in, side_in, ea, side, eb, f2, f3,
                  zs, ys, ops, res, h1, z2, y2, ops2, opse2, res2, rese2, h2,
                  z3, y3, ops3, opse3, res3, rese3):
    zend, yend, xend = (keep(a, lax.axis_size(a)) for a in ("gz", "gy", "gx"))
    low = low_lanes(48)

    @pl.when(jnp.logical_not(early()))
    def _():
        first_half(volume, w, ea, side, zs, ys, ops, res, zend, yend)

    for b in range(2):
        level_one_block(volume, 2 + b, zs, ys, ops, res, w, zend, yend)
        for s in range(10):
            main = res[s * 48 : s * 48 + 48, :128]
            beside = res[s * 48 : s * 48 + 48, 128:]
            if b == 0:
                eb[0, s] = main + jnp.where(low, side[s], 0.0)
                ea[1, s] = ea[1, s] + jnp.where(low, 0.0, beside)
                h1[s] = beside
            else:
                eb[1, s] = main + jnp.where(low, h1[s], 0.0)
                eb[0, s] = eb[0, s] + jnp.where(low, 0.0, beside)
                h1[s] = jnp.where(low, beside * xend[1], side[s] * xend[0])
    next_level([ea.at[0], ea.at[1], eb.at[0], eb.at[1]], h1, z2, y2, ops2, opse2, res2, rese2,
               w, we, f2, h2, 10, 4, 16, 48, 32, zend, yend, xend)
    next_level([f2.at[0], f2.at[1]], h2, z3, y3, ops3, opse3, res3, rese3,
               w, we, f3, None, 7, 2, 8, 32, 32, zend, yend, xend)


def columns_kernel(pa, pb, ea_in, eb_in, f2_in, f3_in, ea, eb, f2, f3, ya, yb, flat):
    odd = lax.rem(lax.axis_index("gx"), 2) == 1
    for j in range(7):
        a, b = pa[3 * j : 3 * j + 3, :], pb[3 * j : 3 * j + 3, :]
        under, over = jnp.where(odd, a, b), jnp.where(odd, b, a)
        full = jnp.concatenate([under[:2], jnp.zeros((125, 128), f32), over[2:]], axis=0)
        flat[j * 128 : j * 128 + 128, :] = full.T
    low = low_lanes(48)
    for s in range(10):
        v = flat[s * 48 : s * 48 + 48, :]
        ea[0, s] = ea[0, s] + jnp.where(low, v, 0.0)
        eb[1, s] = eb[1, s] + jnp.where(low, 0.0, v)
    low = low_lanes(32)
    for s in range(7):
        v = flat[480 + s * 32 : 512 + s * 32, :]
        f2[0, s] = f2[0, s] + jnp.where(low, v, 0.0)
        f2[1, s] = f2[1, s] + jnp.where(low, 0.0, v)
    for s in range(5):
        f3[0, s] = f3[0, s] + flat[704 + s * 32 : 736 + s * 32, :]

    def emit(dst, high):
        for blk in range(4):
            e = ea if blk < 2 else eb
            for s in range(10):
                at = 40 if high else 7
                dst[blk * 10 + s : blk * 10 + s + 1, :] = e[blk % 2, s, at : at + 1, :]
        for j in range(2 if high else 1):
            for blk in range(2):
                for s in range(7):
                    at, to = 24 + j if high else 7, 40 + j * 14 + blk * 7 + s
                    dst[to : to + 1, :] = f2[blk, s, at : at + 1, :]
            for s in range(5):
                at, to = 16 + j if high else 7, 68 + j * 5 + s
                dst[to : to + 1, :] = f3[0, s, at : at + 1, :]

    odd_row = lax.rem(lax.axis_index("gy"), 2) == 1
    for dst, when in ((ya, odd_row), (yb, jnp.logical_not(odd_row))):
        pl.when(when)(lambda dst=dst: emit(dst, False))
        pl.when(jnp.logical_not(when))(lambda dst=dst: emit(dst, True))


def rows_kernel(pa, pb, ea_in, eb_in, f2_in, f3_in, ea, eb, f2, f3, za, zb):
    odd = lax.rem(lax.axis_index("gy"), 2) == 1

    def got(at):
        a, b = pa[at : at + 1, :], pb[at : at + 1, :]
        return jnp.where(odd, a, b), jnp.where(odd, b, a)

    def add(ref, blk, s, at, v):
        ref[blk, s, at : at + 1, :] = ref[blk, s, at : at + 1, :] + v

    for blk in range(4):
        e = ea if blk < 2 else eb
        for s in range(10):
            under, over = got(blk * 10 + s)
            add(e, blk % 2, s, 8, under)
            add(e, blk % 2, s, 39, over)
    for j in range(2):
        for blk in range(2):
            for s in range(7):
                under, over = got(40 + j * 14 + blk * 7 + s)
                add(f2, blk, s, 8 + j, under)
                if j == 0:
                    add(f2, blk, s, 23, over)
        for s in range(5):
            under, over = got(68 + j * 5 + s)
            add(f3, 0, s, 8 + j, under)
            if j == 0:
                add(f3, 0, s, 15, over)

    def emit(dst, high):
        for blk in range(4):
            e = ea if blk < 2 else eb
            dst[blk * 32 : blk * 32 + 32, :] = e[blk % 2, 9 if high else 0, 8:40, :]
        for j in range(2 if high else 1):
            for blk in range(2):
                to = 128 + j * 32 + blk * 16
                dst[to : to + 16, :] = f2[blk, 5 + j if high else 0, 8:24, :]
            to = 192 + j * 8
            dst[to : to + 8, :] = f3[0, 3 + j if high else 0, 8:16, :]

    odd_slab = lax.rem(lax.axis_index("gz"), 2) == 1
    for dst, when in ((za, odd_slab), (zb, jnp.logical_not(odd_slab))):
        pl.when(when)(lambda dst=dst: emit(dst, False))
        pl.when(jnp.logical_not(when))(lambda dst=dst: emit(dst, True))


def inner_kernel(ea, eb, one, held, sem):
    for blk in range(4):
        e = ea if blk < 2 else eb
        for z in range(1, 7):
            held[z - 1, :, blk * 128 : blk * 128 + 128] = e[blk % 2, z + 1, 8:40, :]
    copy = pltpu.make_async_copy(held, one.at[pl.ds(1, 6)], sem)
    copy.start()
    copy.wait()


def sections_kernel(pa, pb, ea, eb, f2, f3, one_in, one, two_out, three_out, held, two, three, sems):
    odd = lax.rem(lax.axis_index("gz"), 2) == 1

    def got(at, tall):
        a, b = pa[at : at + tall, :], pb[at : at + tall, :]
        return jnp.where(odd, a, b), jnp.where(odd, b, a)

    for blk in range(4):
        e = ea if blk < 2 else eb
        under, over = got(blk * 32, 32)
        cols = slice(blk * 128, blk * 128 + 128)
        held[0, :, cols] = e[blk % 2, 1, 8:40, :] + under
        held[1, :, cols] = e[blk % 2, 8, 8:40, :] + over
    copies = [pltpu.make_async_copy(held.at[j], one.at[7 * j], sems.at[j]) for j in range(2)]
    for c in copies:
        c.start()
    for blk in range(2):
        under, over = got(128 + blk * 16, 16)
        further, _ = got(160 + blk * 16, 16)
        for z in range(4):
            v = f2[blk, z + 1, 8:24, :]
            v = v + under if z == 0 else v + further if z == 1 else v + over if z == 3 else v
            two[z, :, blk * 128 : blk * 128 + 128] = v
    under, over = got(192, 8)
    further, _ = got(200, 8)
    three[0] = f3[0, 1, 8:16, :] + under
    three[1] = f3[0, 2, 8:16, :] + further + over
    copies += [
        pltpu.make_async_copy(two, two_out, sems.at[2]),
        pltpu.make_async_copy(three, three_out, sems.at[3]),
    ]
    for c in copies[2:]:
        c.start()
    for c in copies:
        c.wait()


def shape(*dims):
    return jax.ShapeDtypeStruct(dims, f32)


def swap(x, axis, first):
    count = lax.axis_size(axis)
    pairs = []
    for i in range(first, count - 1, 2):
        pairs += [(i, i + 1), (i + 1, i)]
    return lax.ppermute(x, axis, pairs)


def call(kernel, outs, scratch, args, flops, moved, specs=None, aliases=None, limit=16, outs_in=None):
    return pl.pallas_call(
        kernel,
        out_shape=outs,
        in_specs=specs or [VMEM] * len(args),
        out_specs=outs_in or [VMEM] * len(outs),
        scratch_shapes=scratch,
        input_output_aliases=aliases or {},
        compiler_params=pltpu.CompilerParams(vmem_limit_bytes=limit << 20),
        cost_estimate=pl.CostEstimate(flops=flops, bytes_accessed=moved, transcendentals=0),
    )(*args)


def on_device(volume):
    buf = pltpu.VMEM
    levels = [buf((10, 80, 128), f32), buf((7, 48, 128), f32), buf((5, 32, 128), f32)]
    shells, w, we = call(
        shell_kernel,
        [shape(24, 128), jax.ShapeDtypeStruct((768, 256), bf16), jax.ShapeDtypeStruct((384, 256), bf16)],
        [buf((16, 64, 128), f32)] * 3
        + [buf((384, 256), bf16), buf((1024, 384), bf16), buf((1024, 256), f32)]
        + levels
        + [buf((896, 128), f32), pltpu.SemaphoreType.DMA((4,))],
        (volume,),
        10**8,
        1 << 20,
        specs=[pl.BlockSpec(memory_space=pltpu.HBM)],
        limit=50,
    )
    xa = swap(shells, "gx", 0)
    block = [buf((2, 10, 80, 128), f32), buf((2, 10, 48, 128), f32), buf((480, 768), bf16), buf((480, 256), f32)]
    e, f2s, f3s = shape(2, 10, 48, 128), shape(2, 7, 32, 128), shape(1, 5, 32, 128)
    ea, side, again = call(
        first_kernel,
        [e, shape(10, 48, 128), shape(24, 128)],
        block,
        (volume, w, shells),
        4 * 10**9,
        1 << 21,
    )
    xb = swap(again, "gx", 1)
    ea, _, eb, f2, f3 = call(
        second_kernel,
        [e, shape(10, 48, 128), e, f2s, f3s],
        block
        + [buf((10, 48, 128), f32)]
        + [buf((5, 7, 48, 128), f32), buf((5, 7, 32, 128), f32), buf((448, 768), bf16), buf((224, 384), bf16)]
        + [buf((448, 256), f32), buf((224, 256), f32), buf((7, 32, 128), f32)]
        + [buf((3, 5, 32, 128), f32), buf((3, 5, 32, 128), f32), buf((160, 768), bf16), buf((160, 384), bf16)]
        + [buf((160, 256), f32), buf((160, 256), f32)],
        (volume, w, we, ea, side),
        5 * 10**9,
        1 << 21,
        aliases={3: 0, 4: 1},
    )
    keepers = {2: 0, 3: 1, 4: 2, 5: 3}
    ea, eb, f2, f3, ya, yb = call(
        columns_kernel,
        [e, e, f2s, f3s, shape(80, 128), shape(80, 128)],
        [buf((896, 128), f32)],
        (xa, xb, ea, eb, f2, f3),
        10**8,
        1 << 20,
        aliases=keepers,
    )
    ya, yb = swap(ya, "gy", 0), swap(yb, "gy", 1)
    ea, eb, f2, f3, za, zb = call(
        rows_kernel,
        [e, e, f2s, f3s, shape(208, 128), shape(208, 128)],
        [],
        (ya, yb, ea, eb, f2, f3),
        10**8,
        1 << 20,
        aliases=keepers,
    )
    zb = swap(zb, "gz", 1)
    za = swap(za, "gz", 0)
    hbm = pl.BlockSpec(memory_space=pltpu.HBM)
    whole = shape(8, 32, 512)
    (one,) = call(
        inner_kernel,
        [whole],
        [buf((6, 32, 512), f32), pltpu.SemaphoreType.DMA],
        (ea, eb),
        10**8,
        1 << 20,
        outs_in=[hbm],
    )
    return tuple(
        call(
            sections_kernel,
            [whole, shape(4, 16, 256), shape(2, 8, 128)],
            [buf((2, 32, 512), f32), buf((4, 16, 256), f32), buf((2, 8, 128), f32), pltpu.SemaphoreType.DMA((4,))],
            (za, zb, ea, eb, f2, f3, one),
            10**8,
            1 << 20,
            specs=[VMEM] * 6 + [hbm],
            outs_in=[hbm] * 3,
            aliases={6: 0},
        )
    )


def solution(mesh):
    spec = P("gz", "gy", "gx")
    return jax.shard_map(
        on_device, mesh=mesh, in_specs=(spec,), out_specs=(spec,) * 3, check_vma=False
    )
```
